256 devices in a mesh: obs: 64 (over z, y_hi, x), chan: 4 (over y_lo, core).
Axes of the slice: x: 4, y: 4 (y_hi: 2, y_lo: 2; y = y_hi * 2 + y_lo), z: 8, core: 2. Of those that a mesh axis runs over, the one named last changes fastest.
Arguments:
- departures: bfloat16 [8192, 131072], P('chan', 'obs'), may hold values from -8 to 8
- predictors: bfloat16 [10, 131072], P(None, 'obs'), may hold values from -3 to 3
- inv_band: bfloat16 [63, 8192], P(None, 'chan'), may hold values from -1 to 2.5
- band_id: int32 [8192], replicated, may hold values from 0 to 340, never falling along the last dimension, each value on 1 to 32 neighbouring positions
- line_counts: int32 [1024], P('obs'), may hold values from 24 to 128
Outputs:
- gram: float32 [100, 8192], P(None, ('chan', 'obs'))
- rhs: float32 [10, 8192], P(None, ('chan', 'obs'))
The draws below stay inside these ranges and needn't reach their ends.
Inputs may be any that keep to these rules, and one draw needn't show every extreme that they name: `band_id`: band numbers never fall along the channels; a band spans 1 to 32 channels. `line_counts`: slots of a scan line at or beyond its count are empty.
All inputs are finite; a program needn't handle non-finite values.
Results may differ from the reference program's by a relative error of at most 0.00062.
Values may be sent and summed in bfloat16 or wider, within the bound.
A program may use at most 64 MiB of HBM per device.

```python
import math
import jax
import jax.numpy as jnp
import numpy as np
from jax import lax

P_SIZE = 10
C = 8192
MAXB = 32
LINE_SLOTS = 128
LINES = 1024
NOBS = 131072


def draw_inv_band(key, part):
    first_key, second_key = jax.random.split(jax.random.fold_in(key, 17))
    coupling = jnp.clip(0.2 * jax.random.normal(first_key, (2 * MAXB - 1, C), jnp.float32), -1.0, 1.0)
    center = jnp.exp(jax.random.uniform(second_key, (C,), jnp.float32, jnp.log(0.5), jnp.log(2.0)))
    rows_at = jnp.arange(2 * MAXB - 1)[:, None]
    return jnp.where(rows_at == MAXB - 1, center[None, :], coupling).astype(jnp.bfloat16)


def observation_predictors(key):
    value_key = jax.random.fold_in(jax.random.fold_in(key, 101), 1)
    place = jnp.arange(NOBS, dtype=jnp.float32) / jnp.float32(NOBS)
    rising = 0.7 * jnp.exp(jnp.log(3.0) * place)
    level = rising
    values = jax.random.uniform(value_key, (P_SIZE, NOBS), jnp.float32, -1.0, 1.0)
    return values * level[None, :]


def draw_predictors(key, part):
    return observation_predictors(key).astype(jnp.bfloat16)


def draw_departures(key, part):
    pred = observation_predictors(key)
    coef_key, scale_key, noise_key = jax.random.split(jax.random.fold_in(key, 202), 3)
    scales = jnp.exp(jax.random.uniform(scale_key, (C,), jnp.float32, jnp.log(0.2), jnp.log(1.2)))
    coefs = 0.5 * jax.random.normal(coef_key, (C, P_SIZE), jnp.float32) * scales[:, None]
    block = 128
    coef_blocks = coefs.reshape(C // block, block, P_SIZE)

    def one_block(index):
        bias = jnp.dot(coef_blocks[index], pred, precision=lax.Precision.HIGHEST)
        block_key = jax.random.fold_in(noise_key, index)
        noise = 0.5 * jax.random.normal(block_key, (block, NOBS), jnp.float32)
        return jnp.clip(bias + noise, -8.0, 8.0).astype(jnp.bfloat16)
    blocks = lax.map(one_block, jnp.arange(C // block, dtype=jnp.int32))
    return blocks.reshape(C, NOBS)


def set_ends(result, stream_key, smallest, largest):
    shape = result.shape
    spot = [jax.random.randint(jax.random.fold_in(stream_key, axis), (), 0, shape[axis]) for axis in range(len(shape))]
    result = result.at[tuple(spot)].set(smallest)
    longest = shape.index(max(shape))
    spot[longest] = (spot[longest] + 1) % shape[longest]
    return result.at[tuple(spot)].set(largest)


def split_up(count, total, most, skew):
    weights = [(1 << 20) // math.isqrt(grade ** skew) + 1 for grade in range(2, count + 1)]
    surplus, holding = total - most - (count - 1), [1] * (count - 1)
    while surplus > 0:
        free = [i for i in range(count - 1) if holding[i] < most]
        mass, remaining = sum([weights[i] for i in free]), surplus
        for i in free:
            addition = min(most - holding[i], max(1, remaining * weights[i] // mass), surplus)
            holding[i] = holding[i] + addition
            surplus = surplus - addition
    return np.array([most] + holding)


def ragged(stream_key, number_of, total, most, skew):
    if number_of == 2:
        one = jax.random.randint(stream_key, (), max(1, total - most), min(most, total - 1) + 1)
        return jnp.stack([one, total - one])
    lengths = jnp.asarray(split_up(number_of, total, most, skew), jnp.int32)
    pairs = (number_of - 1) // 2
    source_of, receiver = lengths[1:1 + 2 * pairs:2], lengths[2:2 + 2 * pairs:2]
    room = jnp.minimum(source_of - 1, most - receiver)
    shifted = jax.random.randint(jax.random.fold_in(stream_key, 1), (pairs,), 0, 1 << 20) % (room + 1)
    lengths = lengths.at[1:1 + 2 * pairs:2].set(source_of - shifted).at[2:2 + 2 * pairs:2].set(receiver + shifted)
    return lengths[jax.random.permutation(jax.random.fold_in(stream_key, 2), number_of)]


def setup_inputs(seed: int = 0) -> dict:
    streams_of = jax.random.split(jax.random.key(seed), 6)
    departures = draw_departures(jax.random.fold_in(streams_of[5], 71), 0)
    predictors = draw_predictors(jax.random.fold_in(streams_of[5], 71), 0)
    inv_band = draw_inv_band(jax.random.fold_in(streams_of[5], 71), 0)
    band_id = jnp.searchsorted(jnp.cumsum(ragged(streams_of[3], C // 24, C, MAXB, 1)), jnp.arange(C), side="right").astype(jnp.int32)
    line_counts = set_ends(jax.random.randint(streams_of[4], (LINES,), 24, LINE_SLOTS + 1), jax.random.fold_in(streams_of[4], 1), 24, LINE_SLOTS).astype(jnp.int32)
    return {"departures": departures, "predictors": predictors, "inv_band": inv_band, "band_id": band_id, "line_counts": line_counts}


huber_edge = 1.0


def reference(departures, predictors, inv_band, band_id, line_counts):
    chans, nobs = departures.shape
    half = MAXB - 1
    tile = 128
    extent = tile + 2 * half
    slots = jnp.arange(nobs, dtype=jnp.int32)
    live = (slots % LINE_SLOTS < jnp.repeat(line_counts, LINE_SLOTS)).astype(jnp.float32)
    pred_wide = predictors.astype(jnp.float32).T
    pairs_t = (pred_wide[:, :, None] * pred_wide[:, None, :]).reshape(nobs, P_SIZE * P_SIZE).astype(jnp.bfloat16)
    pred_t = predictors.T

    def one_tile(index):
        first = index * tile
        start = jnp.clip(first - half, 0, chans - extent).astype(jnp.int32)
        rows_at = first + jnp.arange(tile, dtype=jnp.int32)
        cols_at = start + jnp.arange(extent, dtype=jnp.int32)
        offset = cols_at[None, :] - rows_at[:, None] + half
        keep = (offset >= 0) & (offset <= 2 * half) & (band_id[cols_at][None, :] == band_id[rows_at][:, None])
        values = inv_band[jnp.clip(offset, 0, 2 * half), rows_at[:, None]]
        matrix = jnp.where(keep, values, jnp.zeros_like(values))
        window = lax.dynamic_slice_in_dim(departures, start, extent, 0)
        weighted = jnp.dot(matrix, window, preferred_element_type=jnp.float32)
        ratio = live[None, :] * (huber_edge / jnp.maximum(jnp.abs(weighted), huber_edge))
        qc_weight = ratio.astype(jnp.bfloat16)
        scaled = (ratio * weighted).astype(jnp.bfloat16)
        gram_tile = jnp.dot(qc_weight, pairs_t, preferred_element_type=jnp.float32)
        rhs_tile = jnp.dot(scaled, pred_t, preferred_element_type=jnp.float32)
        return gram_tile, rhs_tile

    grams, rhss = lax.map(one_tile, jnp.arange(chans // tile, dtype=jnp.int32))
    gram = grams.reshape(chans, P_SIZE * P_SIZE).T / jnp.float32(nobs)
    rhs = rhss.reshape(chans, P_SIZE).T / jnp.float32(nobs)
    return gram, rhs
```

```python
import functools

import jax
import jax.numpy as jnp
import numpy as np
from jax import lax
from jax.experimental import pallas as pl
from jax.experimental.pallas import tpu as pltpu
from jax.sharding import PartitionSpec as P

MESH = pl.DeviceIdType.MESH
PRED = 10
HALO = 32
BLOCK = 256
WINDOW = 192
PAIRS = [(j, k) for j in range(PRED) for k in range(j, PRED)]
MAIN = 64


def selectors():
    left = np.zeros((16, 128), np.float32)
    right = np.zeros((16, 128), np.float32)
    alone = np.zeros((16, 256), np.float32)
    for half in range(2):
        for m, (j, k) in enumerate(PAIRS):
            left[j, half * MAIN + m] = 1
            right[k, half * MAIN + m] = 1
        for k in range(PRED - 1):
            alone[k, half * MAIN + len(PAIRS) + k] = 1
    alone[PRED - 1, 128:] = 1
    return np.concatenate([left, right, alone], axis=1)


def kernel(
    dep_ref, pred_ref, inv_ref, ids_ref, lines_ref, sel_ref,
    gram_ref, rhs_ref,
    cells, wq, ws, inv_t, id_rows, id_cols, send1, recv1, own, send2, recv2,
    load_sem, halo_send, halo_recv, send1_sem, recv1_sem, send2_sem, recv2_sem,
):
    obs = lax.axis_index("obs")
    chan = lax.axis_index("chan")
    z, p = obs // 8, obs % 8
    rows = dep_ref.shape[0]
    blocks = rows // BLOCK
    factor = 1.0 / float(dep_ref.shape[1] * lax.axis_size("obs"))
    last = lax.axis_size("chan") - 1
    turn = 1 - 2 * (z // 4)

    def block_at(step):
        return (z + turn * (step + 1) + 2 * blocks) % blocks

    def load(number):
        at = pl.multiple_of(number * BLOCK, BLOCK)
        return pltpu.make_async_copy(
            dep_ref.at[pl.ds(at, BLOCK)],
            cells.at[pl.ds(pl.multiple_of(at + HALO, HALO), BLOCK)],
            load_sem.at[number],
        )

    def piece(order):
        return (z + turn * order + 2 * blocks) % blocks

    for order in range(blocks):
        load(piece(order)).start()

    barrier = pltpu.get_barrier_semaphore()
    for d in range(1, 8):
        pl.semaphore_signal(barrier, inc=1, device_id=((z + d) % 8 * 8 + p, chan), device_id_type=MESH)
        pl.semaphore_signal(barrier, inc=1, device_id=(z * 8 + (p + d) % 8, chan), device_id_type=MESH)

    @pl.when(chan > 0)
    def _():
        pl.semaphore_signal(barrier, inc=1, device_id=(obs, chan - 1), device_id_type=MESH)

    @pl.when(chan < last)
    def _():
        pl.semaphore_signal(barrier, inc=1, device_id=(obs, chan + 1), device_id_type=MESH)

    here = pl.multiple_of(chan * 16, 16)
    id_rows[pl.ds(8, 16), :] = ids_ref[pl.ds(here, 16), :].astype(jnp.float32)
    before = ids_ref[pl.ds(jnp.maximum(here - 1, 0), 1), :].astype(jnp.float32)
    after = ids_ref[pl.ds(jnp.minimum(here + 16, 16 * last + 15), 1), :].astype(jnp.float32)
    id_rows[pl.ds(7, 1), :] = jnp.where(chan > 0, before, -1.0)
    id_rows[pl.ds(24, 1), :] = jnp.where(chan < last, after, -1.0)
    lane16 = lax.broadcasted_iota(jnp.int32, (16, 128), 1)
    turned = [pltpu.roll(id_rows[pl.ds(7 + n, 16), :], 32, axis=1) for n in range(3)]
    id_cols[:, 0:128] = jnp.where(lane16 < 32, turned[0], turned[1])
    id_cols[:, 128:256] = jnp.where(lane16 < 32, turned[1], turned[2])

    @pl.loop(0, 16)
    def _(s):
        at = pl.multiple_of(s * 128, 128)
        entries = inv_ref[:, pl.ds(at, 128)].astype(jnp.float32)
        number = jnp.broadcast_to(id_rows[pl.ds(8 + s, 1), :], (64, 128))
        stacked = jnp.concatenate([entries, jnp.zeros((1, 128), jnp.float32), number], axis=0)
        inv_t[pl.ds(at, 128), :] = stacked.T

    @pl.loop(0, 16)
    def _(s):
        at = pl.multiple_of(s * 128, 128)
        lane = lax.broadcasted_iota(jnp.int32, (PRED, 128), 1)
        values = pred_ref[:, pl.ds(at, 128)].astype(jnp.float32)
        values = jnp.where(lane < lines_ref[s], values, 0.0)
        values = jnp.concatenate([values, jnp.zeros((16 - PRED, 128), jnp.float32)], axis=0)
        picked = jnp.dot(
            values.T.astype(jnp.bfloat16), sel_ref[...], preferred_element_type=jnp.float32
        )
        products = (picked[:, 0:128] * picked[:, 128:256]).astype(jnp.bfloat16)
        wq[pl.ds(at, 128), :] = jnp.concatenate([products, jnp.zeros_like(products)], axis=1)
        ws[pl.ds(at, 128), :] = picked[:, 256:512].astype(jnp.bfloat16)

    pl.semaphore_wait(barrier, 14 + jnp.minimum(chan, 1) + jnp.minimum(last - chan, 1))

    def up():
        return pltpu.make_async_remote_copy(
            src_ref=dep_ref.at[pl.ds(0, HALO)],
            dst_ref=cells.at[pl.ds(HALO + rows, HALO)],
            send_sem=halo_send.at[0],
            recv_sem=halo_recv.at[0],
            device_id=(obs, jnp.maximum(chan - 1, 0)),
            device_id_type=MESH,
        )

    def down():
        return pltpu.make_async_remote_copy(
            src_ref=dep_ref.at[pl.ds(rows - HALO, HALO)],
            dst_ref=cells.at[pl.ds(0, HALO)],
            send_sem=halo_send.at[1],
            recv_sem=halo_recv.at[1],
            device_id=(obs, jnp.minimum(chan + 1, last)),
            device_id_type=MESH,
        )

    @pl.when(chan > 0)
    def _():
        up().start()

    @pl.when(chan < last)
    def _():
        down().start()

    @pl.when(chan == 0)
    def _():
        cells[pl.ds(0, HALO), :] = jnp.zeros((HALO, cells.shape[1]), jnp.bfloat16)

    @pl.when(chan == last)
    def _():
        cells[pl.ds(HALO + rows, HALO), :] = jnp.zeros((HALO, cells.shape[1]), jnp.bfloat16)

    def to_plane(number):
        return pltpu.make_async_remote_copy(
            src_ref=send1.at[number],
            dst_ref=recv1.at[z],
            send_sem=send1_sem,
            recv_sem=recv1_sem,
            device_id=(number * 8 + p, chan),
            device_id_type=MESH,
        )

    def band(first):
        lane = lax.broadcasted_iota(jnp.int32, (128, 128), 1)
        both = inv_t[pl.ds(first, 128), :]
        entries = jnp.where(lane < 64, both, 0.0)
        number = jnp.where(lane < 64, pltpu.roll(both, 64, axis=1), both)
        wide = jnp.concatenate([entries, jnp.zeros_like(entries)], axis=1)
        wide = pltpu.roll(wide, 1, axis=1, stride=1, stride_axis=0)
        near = id_cols[pl.ds(first // 128, 1), :]
        same = jnp.concatenate([number, number], axis=1) == near
        return jnp.where(same, wide, 0.0).astype(jnp.bfloat16)[:, 0:WINDOW]

    load(piece(0)).wait()
    load(piece(1)).wait()

    @pl.loop(0, blocks)
    def _(step):
        number = block_at(step)

        @pl.when(step < blocks - 2)
        def _():
            load(piece(step + 2)).wait()

        @pl.when((number == 0) & (chan > 0))
        def _():
            down().wait_recv()

        @pl.when((number == blocks - 1) & (chan < last))
        def _():
            up().wait_recv()

        first = pl.multiple_of(number * BLOCK, BLOCK)
        matrices = [band(first + 128 * n) for n in range(2)]
        total = jnp.zeros((BLOCK, 256), jnp.float32)
        for part in range(cells.shape[1] // 256):
            cols = pl.ds(part * 256, 256)
            weighted = jnp.concatenate(
                [
                    jnp.dot(
                        matrices[n],
                        cells[pl.ds(pl.multiple_of(first + 128 * n, 128), WINDOW), cols],
                        preferred_element_type=jnp.float32,
                    )
                    for n in range(2)
                ],
                axis=0,
            )
            weight = (1.0 / jnp.maximum(jnp.abs(weighted), 1.0)).astype(jnp.bfloat16)
            scaled = jnp.clip(weighted, -1.0, 1.0).astype(jnp.bfloat16)
            total = total + jnp.dot(weight, wq[cols, :], preferred_element_type=jnp.float32)
            total = total + jnp.dot(scaled, ws[cols, :], preferred_element_type=jnp.float32)

        lane = lax.broadcasted_iota(jnp.int32, (8, 16, 128), 2)
        halves = total[:, 0:128].reshape(8, 2, 16, 128)
        main = jnp.where(lane < MAIN, halves[:, 0], halves[:, 1]).reshape(16, 8, 128)
        tenth = total[:, 128:256].reshape(8, 32, 128)
        on = lax.broadcasted_iota(jnp.int32, (8, 32, 128), 2) == lax.broadcasted_iota(
            jnp.int32, (8, 32, 128), 1
        )
        tenth = jnp.sum(jnp.where(on, tenth, 0.0), axis=1)
        own[0:16] = main
        own[16] = tenth
        send1[number, 0:16] = main.astype(jnp.bfloat16)
        send1[number, 16] = tenth.astype(jnp.bfloat16)

        @pl.when(step < blocks - 1)
        def _():
            to_plane(number).start()

    def wait_for(buffer, sem):
        pltpu.make_async_copy(buffer.at[pl.ds(0, 7)], buffer.at[pl.ds(0, 7)], sem).wait()

    wait_for(recv1, recv1_sem)
    sums = own[...]
    for source in range(8):
        came = recv1[source].astype(jnp.float32)
        sums = sums + jnp.where(source == z, jnp.zeros_like(came), came)
    for peer in range(8):
        send2[peer, 0:2] = sums[2 * peer : 2 * peer + 2]
        send2[peer, 2] = sums[16]

    @pl.loop(1, 8)
    def _(d):
        peer = (p + d) % 8
        pltpu.make_async_remote_copy(
            src_ref=send2.at[peer],
            dst_ref=recv2.at[p],
            send_sem=send2_sem,
            recv_sem=recv2_sem,
            device_id=(z * 8 + peer, chan),
            device_id_type=MESH,
        ).start()

    mine = send2[p]
    wait_for(recv2, recv2_sem)
    whole = mine
    for source in range(8):
        came = recv2[source]
        whole = whole + jnp.where(source == p, jnp.zeros_like(came), came)
    whole = whole * factor
    flat = whole[0:2].reshape(16, 128).T
    values = jnp.concatenate([flat[0:MAIN], flat[MAIN:128]], axis=1)
    index = {pair: m for m, pair in enumerate(PAIRS)}
    for j in range(PRED):
        for k in range(PRED):
            m = index[(min(j, k), max(j, k))]
            gram_ref[pl.ds(j * PRED + k, 1), :] = values[m : m + 1, :]
    rhs_ref[0 : PRED - 1, :] = values[len(PAIRS) : MAIN, :]
    row = lax.broadcasted_iota(jnp.int32, (8, 128), 0)
    tenth = jnp.sum(jnp.where(row == p, whole[2], 0.0), axis=0, keepdims=True)
    rhs_ref[PRED - 1 : PRED, :] = tenth[:, 0:32]

    wait_for(send1, send1_sem)
    wait_for(send2, send2_sem)

    @pl.when(chan > 0)
    def _():
        up().wait_send()

    @pl.when(chan < last)
    def _():
        down().wait_send()


def on_device(departures, predictors, inv_band, band_id, line_counts):
    rows, obs_dev = departures.shape
    owned = rows // lax.axis_size("obs")
    vmem = pl.BlockSpec(memory_space=pltpu.VMEM)
    return pl.pallas_call(
        kernel,
        out_shape=(
            jax.ShapeDtypeStruct((PRED * PRED, owned), jnp.float32),
            jax.ShapeDtypeStruct((PRED, owned), jnp.float32),
        ),
        in_specs=[
            pl.BlockSpec(memory_space=pltpu.HBM),
            vmem,
            vmem,
            vmem,
            pl.BlockSpec(memory_space=pltpu.SMEM),
            vmem,
        ],
        out_specs=(vmem, vmem),
        scratch_shapes=[
            pltpu.VMEM((rows + 2 * HALO, obs_dev), jnp.bfloat16),
            pltpu.VMEM((obs_dev, 256), jnp.bfloat16),
            pltpu.VMEM((obs_dev, 256), jnp.bfloat16),
            pltpu.VMEM((rows, 128), jnp.float32),
            pltpu.VMEM((32, 128), jnp.float32),
            pltpu.VMEM((16, 256), jnp.float32),
            pltpu.VMEM((8, 17, 8, 128), jnp.bfloat16),
            pltpu.VMEM((8, 17, 8, 128), jnp.bfloat16),
            pltpu.VMEM((17, 8, 128), jnp.float32),
            pltpu.VMEM((8, 3, 8, 128), jnp.float32),
            pltpu.VMEM((8, 3, 8, 128), jnp.float32),
            pltpu.SemaphoreType.DMA((8,)),
            pltpu.SemaphoreType.DMA((2,)),
            pltpu.SemaphoreType.DMA((2,)),
            pltpu.SemaphoreType.DMA,
            pltpu.SemaphoreType.DMA,
            pltpu.SemaphoreType.DMA,
            pltpu.SemaphoreType.DMA,
        ],
        compiler_params=pltpu.CompilerParams(collective_id=0, has_side_effects=True),
        name="normal_equations",
    )(
        departures,
        predictors,
        inv_band,
        band_id.reshape(band_id.shape[0] // 128, 128),
        line_counts,
        jnp.asarray(selectors(), jnp.bfloat16),
    )


def solution(mesh):
    in_specs = (P("chan", "obs"), P(None, "obs"), P(None, "chan"), P(), P("obs"))
    out_specs = (P(None, ("chan", "obs")), P(None, ("chan", "obs")))
    return jax.shard_map(
        on_device, mesh=mesh, in_specs=in_specs, out_specs=out_specs, check_vma=False
    )
```

```python
import functools

import jax
import jax.numpy as jnp
import numpy as np
from jax import lax
from jax.experimental import pallas as pl
from jax.experimental.pallas import tpu as pltpu
from jax.sharding import PartitionSpec as P

MESH = pl.DeviceIdType.MESH
PRED = 10
HALO = 32
BLOCK = 256
WINDOW = 192
PAIRS = [(j, k) for j in range(PRED) for k in range(j, PRED)]
MAIN = 64


def selectors():
    left = np.zeros((16, 128), np.float32)
    right = np.zeros((16, 128), np.float32)
    alone = np.zeros((16, 256), np.float32)
    for half in range(2):
        for m, (j, k) in enumerate(PAIRS):
            left[j, half * MAIN + m] = 1
            right[k, half * MAIN + m] = 1
        for k in range(PRED - 1):
            alone[k, half * MAIN + len(PAIRS) + k] = 1
    alone[PRED - 1, 128:] = 1
    return np.concatenate([left, right, alone], axis=1)


def kernel(
    dep_ref, pred_hbm, inv_hbm, ids_hbm, lines_hbm, sel_hbm,
    gram_ref, rhs_ref,
    cells, pred_ref, inv_ref, ids_ref, lines_ref, sel_ref,
    wq, ws, id_rows, id_cols, mat_a, mat_b, weight0, scaled0,
    send1, recv1, own, send2, recv2,
    small_sem, load_sem, halo_send, halo_recv, send1_sem, recv1_sem, send2_sem, recv2_sem,
):
    obs = lax.axis_index("obs")
    chan = lax.axis_index("chan")
    z, p = obs // 8, obs % 8
    rows = dep_ref.shape[0]
    blocks = rows // BLOCK
    parts = cells.shape[1] // 256
    factor = 1.0 / float(dep_ref.shape[1] * lax.axis_size("obs"))
    last = lax.axis_size("chan") - 1
    turn = 1 - 2 * (z // 4)

    barrier = pltpu.get_barrier_semaphore()

    @pl.when(chan > 0)
    def _():
        pl.semaphore_signal(barrier, inc=1, device_id=(obs, chan - 1), device_id_type=MESH)

    @pl.when(chan < last)
    def _():
        pl.semaphore_signal(barrier, inc=1, device_id=(obs, chan + 1), device_id_type=MESH)

    smalls = [
        pltpu.make_async_copy(source, target, small_sem.at[n])
        for n, (source, target) in enumerate(
            [
                (pred_hbm, pred_ref),
                (lines_hbm, lines_ref),
                (sel_hbm, sel_ref),
                (ids_hbm, ids_ref),
                (inv_hbm, inv_ref),
            ]
        )
    ]
    for copy in smalls:
        copy.start()

    def piece(order):
        return (z + turn * order + 2 * blocks) % blocks

    def load(order):
        number = piece(order)
        at = pl.multiple_of(number * BLOCK, BLOCK)
        return pltpu.make_async_copy(
            dep_ref.at[pl.ds(at, BLOCK)],
            cells.at[pl.ds(pl.multiple_of(at + HALO, HALO), BLOCK)],
            load_sem.at[order],
        )

    for order in range(blocks):
        load(order).start()

    for d in range(1, 8):
        pl.semaphore_signal(barrier, inc=1, device_id=((z + d) % 8 * 8 + p, chan), device_id_type=MESH)
        pl.semaphore_signal(barrier, inc=1, device_id=(z * 8 + (p + d) % 8, chan), device_id_type=MESH)

    @pl.when(chan == 0)
    def _():
        cells[pl.ds(0, HALO), :] = jnp.zeros((HALO, cells.shape[1]), jnp.bfloat16)

    @pl.when(chan == last)
    def _():
        cells[pl.ds(HALO + rows, HALO), :] = jnp.zeros((HALO, cells.shape[1]), jnp.bfloat16)

    for copy in smalls:
        copy.wait()

    here = pl.multiple_of(chan * 16, 16)
    id_rows[pl.ds(8, 16), :] = ids_ref[pl.ds(here, 16), :].astype(jnp.float32)
    before = ids_ref[pl.ds(jnp.maximum(here - 1, 0), 1), :].astype(jnp.float32)
    after = ids_ref[pl.ds(jnp.minimum(here + 16, 16 * last + 15), 1), :].astype(jnp.float32)
    id_rows[pl.ds(7, 1), :] = jnp.where(chan > 0, before, -1.0)
    id_rows[pl.ds(24, 1), :] = jnp.where(chan < last, after, -1.0)
    lane16 = lax.broadcasted_iota(jnp.int32, (16, 128), 1)
    turned = [pltpu.roll(id_rows[pl.ds(7 + n, 16), :], 32, axis=1) for n in range(3)]
    id_cols[:, 0:128] = jnp.where(lane16 < 32, turned[0], turned[1])
    id_cols[:, 128:256] = jnp.where(lane16 < 32, turned[1], turned[2])

    for s in range(cells.shape[1] // 128):
        lane = lax.broadcasted_iota(jnp.int32, (PRED, 128), 1)
        values = pred_ref[:, s * 128 : s * 128 + 128].astype(jnp.float32)
        values = jnp.where(lane < lines_ref[s], values, 0.0)
        values = jnp.concatenate([values, jnp.zeros((16 - PRED, 128), jnp.float32)], axis=0)
        picked = jnp.dot(
            values.T.astype(jnp.bfloat16), sel_ref[...], preferred_element_type=jnp.float32
        )
        products = (picked[:, 0:128] * picked[:, 128:256]).astype(jnp.bfloat16)
        wq[pl.ds(s * 128, 128), :] = jnp.concatenate([products, jnp.zeros_like(products)], axis=1)
        ws[pl.ds(s * 128, 128), :] = picked[:, 256:512].astype(jnp.bfloat16)

    def band(first):
        block = first // 128
        entries = inv_ref[:, pl.ds(first, 128)].astype(jnp.float32)
        number = jnp.broadcast_to(id_rows[pl.ds(8 + block, 1), :], (64, 128))
        both = jnp.concatenate([entries, jnp.zeros((1, 128), jnp.float32), number], axis=0).T
        lane = lax.broadcasted_iota(jnp.int32, (128, 128), 1)
        entries = jnp.where(lane < 64, both, 0.0)
        number = jnp.where(lane < 64, pltpu.roll(both, 64, axis=1), both)
        wide = jnp.concatenate([entries, jnp.zeros_like(entries)], axis=1)
        wide = pltpu.roll(wide, 1, axis=1, stride=1, stride_axis=0)
        near = id_cols[pl.ds(block, 1), :]
        same = jnp.concatenate([number, number], axis=1) == near
        return jnp.where(same, wide, 0.0).astype(jnp.bfloat16)

    def start_of(number):
        return pl.multiple_of(number * BLOCK, BLOCK)

    def make(number, mat):
        for n in range(2):
            mat[n] = band(pl.multiple_of(start_of(number) + 128 * n, 128))

    def product(number, mat, part):
        first = start_of(number)
        cols = pl.ds(part * 256, 256)
        return [
            jnp.dot(
                mat[n][:, 0:WINDOW],
                cells[pl.ds(pl.multiple_of(first + 128 * n, 128), WINDOW), cols],
                preferred_element_type=jnp.float32,
            )
            for n in range(2)
        ]

    def weigh(weighted):
        weight = [(1.0 / jnp.maximum(jnp.abs(w), 1.0)).astype(jnp.bfloat16) for w in weighted]
        scaled = [jnp.clip(w, -1.0, 1.0).astype(jnp.bfloat16) for w in weighted]
        return jnp.concatenate(weight, axis=0), jnp.concatenate(scaled, axis=0)

    for order in range(3):
        load(order).wait()
    make(piece(1), mat_a)
    weight0[...], scaled0[...] = weigh(product(piece(1), mat_a, 0))

    pl.semaphore_wait(barrier, 14 + jnp.minimum(chan, 1) + jnp.minimum(last - chan, 1))

    def up():
        return pltpu.make_async_remote_copy(
            src_ref=dep_ref.at[pl.ds(0, HALO)],
            dst_ref=cells.at[pl.ds(HALO + rows, HALO)],
            send_sem=halo_send.at[0],
            recv_sem=halo_recv.at[0],
            device_id=(obs, jnp.maximum(chan - 1, 0)),
            device_id_type=MESH,
        )

    def down():
        return pltpu.make_async_remote_copy(
            src_ref=dep_ref.at[pl.ds(rows - HALO, HALO)],
            dst_ref=cells.at[pl.ds(0, HALO)],
            send_sem=halo_send.at[1],
            recv_sem=halo_recv.at[1],
            device_id=(obs, jnp.minimum(chan + 1, last)),
            device_id_type=MESH,
        )

    @pl.when(chan > 0)
    def _():
        up().start()

    @pl.when(chan < last)
    def _():
        down().start()

    def to_plane(number):
        return pltpu.make_async_remote_copy(
            src_ref=send1.at[number],
            dst_ref=recv1.at[z],
            send_sem=send1_sem,
            recv_sem=recv1_sem,
            device_id=(number * 8 + p, chan),
            device_id_type=MESH,
        )

    def block_step(step, mat, mat_next):
        number, following = piece(step + 1), piece(step + 2)

        @pl.when(step < blocks - 3)
        def _():
            load(step + 3).wait()

        @pl.when((following == 0) & (chan > 0))
        def _():
            down().wait_recv()

        @pl.when((following == blocks - 1) & (chan < last))
        def _():
            up().wait_recv()

        make(following, mat_next)
        total = jnp.zeros((BLOCK, 256), jnp.float32)
        weight, scaled = weight0[...], scaled0[...]
        for part in range(parts):
            if part < parts - 1:
                coming = product(number, mat, part + 1)
            else:
                coming = product(following, mat_next, 0)
            cols = pl.ds(part * 256, 256)
            total = total + jnp.dot(weight, wq[cols, :], preferred_element_type=jnp.float32)
            total = total + jnp.dot(scaled, ws[cols, :], preferred_element_type=jnp.float32)
            weight, scaled = weigh(coming)
        weight0[...], scaled0[...] = weight, scaled

        lane = lax.broadcasted_iota(jnp.int32, (8, 16, 128), 2)
        halves = total[:, 0:128].reshape(8, 2, 16, 128)
        main = jnp.where(lane < MAIN, halves[:, 0], halves[:, 1]).reshape(16, 8, 128)
        tenth = total[:, 128:256].reshape(8, 32, 128)
        on = lax.broadcasted_iota(jnp.int32, (8, 32, 128), 2) == lax.broadcasted_iota(
            jnp.int32, (8, 32, 128), 1
        )
        tenth = jnp.sum(jnp.where(on, tenth, 0.0), axis=1)
        own[0:16] = main
        own[16] = tenth
        send1[number, 0:16] = main.astype(jnp.bfloat16)
        send1[number, 16] = tenth.astype(jnp.bfloat16)

        @pl.when(step < blocks - 1)
        def _():
            to_plane(number).start()

    @pl.loop(0, blocks // 2)
    def _(pair):
        block_step(2 * pair, mat_a, mat_b)
        block_step(2 * pair + 1, mat_b, mat_a)

    def wait_for(buffer, sem):
        pltpu.make_async_copy(buffer.at[pl.ds(0, 7)], buffer.at[pl.ds(0, 7)], sem).wait()

    wait_for(recv1, recv1_sem)
    sums = own[...]
    for source in range(8):
        came = recv1[source].astype(jnp.float32)
        sums = sums + jnp.where(source == z, jnp.zeros_like(came), came)
    for peer in range(8):
        send2[peer, 0:2] = sums[2 * peer : 2 * peer + 2]
        send2[peer, 2] = sums[16]

    @pl.loop(1, 8)
    def _(d):
        peer = (p + d) % 8
        pltpu.make_async_remote_copy(
            src_ref=send2.at[peer],
            dst_ref=recv2.at[p],
            send_sem=send2_sem,
            recv_sem=recv2_sem,
            device_id=(z * 8 + peer, chan),
            device_id_type=MESH,
        ).start()

    mine = send2[p]
    wait_for(recv2, recv2_sem)
    whole = mine
    for source in range(8):
        came = recv2[source]
        whole = whole + jnp.where(source == p, jnp.zeros_like(came), came)
    whole = whole * factor
    flat = whole[0:2].reshape(16, 128).T
    values = jnp.concatenate([flat[0:MAIN], flat[MAIN:128]], axis=1)
    index = {pair: m for m, pair in enumerate(PAIRS)}
    for j in range(PRED):
        for k in range(PRED):
            m = index[(min(j, k), max(j, k))]
            gram_ref[pl.ds(j * PRED + k, 1), :] = values[m : m + 1, :]
    rhs_ref[0 : PRED - 1, :] = values[len(PAIRS) : MAIN, :]
    row = lax.broadcasted_iota(jnp.int32, (8, 128), 0)
    tenth = jnp.sum(jnp.where(row == p, whole[2], 0.0), axis=0, keepdims=True)
    rhs_ref[PRED - 1 : PRED, :] = tenth[:, 0:32]

    wait_for(send1, send1_sem)
    wait_for(send2, send2_sem)

    @pl.when(chan > 0)
    def _():
        up().wait_send()

    @pl.when(chan < last)
    def _():
        down().wait_send()


def on_device(departures, predictors, inv_band, band_id, line_counts):
    rows, obs_dev = departures.shape
    owned = rows // lax.axis_size("obs")
    vmem = pl.BlockSpec(memory_space=pltpu.VMEM)
    return pl.pallas_call(
        kernel,
        out_shape=(
            jax.ShapeDtypeStruct((PRED * PRED, owned), jnp.float32),
            jax.ShapeDtypeStruct((PRED, owned), jnp.float32),
        ),
        in_specs=[pl.BlockSpec(memory_space=pltpu.HBM)] * 6,
        out_specs=(vmem, vmem),
        scratch_shapes=[
            pltpu.VMEM((rows + 2 * HALO, obs_dev), jnp.bfloat16),
            pltpu.VMEM(predictors.shape, jnp.bfloat16),
            pltpu.VMEM(inv_band.shape, jnp.bfloat16),
            pltpu.VMEM((band_id.shape[0] // 128, 128), jnp.int32),
            pltpu.SMEM(line_counts.shape, jnp.int32),
            pltpu.VMEM((16, 512), jnp.bfloat16),
            pltpu.VMEM((obs_dev, 256), jnp.bfloat16),
            pltpu.VMEM((obs_dev, 256), jnp.bfloat16),
            pltpu.VMEM((32, 128), jnp.float32),
            pltpu.VMEM((16, 256), jnp.float32),
            pltpu.VMEM((2, 128, 256), jnp.bfloat16),
            pltpu.VMEM((2, 128, 256), jnp.bfloat16),
            pltpu.VMEM((BLOCK, 256), jnp.bfloat16),
            pltpu.VMEM((BLOCK, 256), jnp.bfloat16),
            pltpu.VMEM((8, 17, 8, 128), jnp.bfloat16),
            pltpu.VMEM((8, 17, 8, 128), jnp.bfloat16),
            pltpu.VMEM((17, 8, 128), jnp.float32),
            pltpu.VMEM((8, 3, 8, 128), jnp.float32),
            pltpu.VMEM((8, 3, 8, 128), jnp.float32),
            pltpu.SemaphoreType.DMA((5,)),
            pltpu.SemaphoreType.DMA((8,)),
            pltpu.SemaphoreType.DMA((2,)),
            pltpu.SemaphoreType.DMA((2,)),
            pltpu.SemaphoreType.DMA,
            pltpu.SemaphoreType.DMA,
            pltpu.SemaphoreType.DMA,
            pltpu.SemaphoreType.DMA,
        ],
        compiler_params=pltpu.CompilerParams(collective_id=0, has_side_effects=True),
        name="normal_equations",
    )(
        departures,
        predictors,
        inv_band,
        band_id.reshape(band_id.shape[0] // 128, 128),
        line_counts,
        jnp.asarray(selectors(), jnp.bfloat16),
    )


def solution(mesh):
    in_specs = (P("chan", "obs"), P(None, "obs"), P(None, "chan"), P(), P("obs"))
    out_specs = (P(None, ("chan", "obs")), P(None, ("chan", "obs")))
    return jax.shard_map(
        on_device, mesh=mesh, in_specs=in_specs, out_specs=out_specs, check_vma=False
    )
```

```python
import functools

import jax
import jax.numpy as jnp
import numpy as np
from jax import lax
from jax.experimental import pallas as pl
from jax.experimental.pallas import tpu as pltpu
from jax.sharding import PartitionSpec as P

MESH = pl.DeviceIdType.MESH
PRED = 10
HALO = 32
BLOCK = 256
WINDOW = 192
PAIRS = [(j, k) for j in range(PRED) for k in range(j, PRED)]
HALF = 64
TILES = 19

ORDERS = (
    (5, 6, 2, 1, 7, 3, 4, 0),
    (5, 2, 6, 7, 3, 0, 4, 1),
    (5, 6, 4, 0, 7, 1, 3, 2),
    (2, 6, 1, 4, 7, 5, 0, 3),
    (3, 2, 1, 7, 0, 6, 5, 4),
    (1, 4, 2, 6, 0, 3, 7, 5),
    (1, 5, 2, 0, 3, 7, 4, 6),
    (4, 1, 3, 0, 6, 5, 2, 7),
)


def loads_of(order):
    needed = []
    for block in order:
        for near in (block - 1, block, block + 1):
            if 0 <= near < len(order) and near not in needed:
                needed.append(near)
    return tuple(needed)


def code_of(order):
    return sum(block * 8**n for n, block in enumerate(order))


def pick(z, codes):
    code = jnp.int32(codes[0])
    for n in range(1, len(codes)):
        code = jnp.where(z == n, jnp.int32(codes[n]), code)
    return code


def selectors():
    left = np.zeros((16, 128), np.float32)
    right = np.zeros((16, 128), np.float32)
    for half in range(2):
        for m, (j, k) in enumerate(PAIRS):
            left[j, half * HALF + m] = 1
            right[k, half * HALF + m] = 1
    return np.concatenate([left, right], axis=1)


def kernel(
    dep_ref, pred_hbm, inv_hbm, ids_hbm, lines_hbm, sel_hbm,
    gram_ref, rhs_ref,
    cells, pred_ref, inv_ref, ids_ref, lines_ref, sel_ref,
    wq, live_pred, id_rows, id_cols, mat_a, mat_b, weight0, scaled0,
    send1, recv1, own, send2, recv2,
    small_sem, load_sem, halo_send, halo_recv, send1_sem, recv1_sem, send2_sem, recv2_sem,
):
    obs = lax.axis_index("obs")
    chan = lax.axis_index("chan")
    z, p = obs // 8, obs % 8
    rows = dep_ref.shape[0]
    blocks = rows // BLOCK
    parts = cells.shape[1] // 256
    factor = 1.0 / float(dep_ref.shape[1] * lax.axis_size("obs"))
    last = lax.axis_size("chan") - 1
    order_code = pick(z, [code_of(order + order[:1]) for order in ORDERS])
    load_code = pick(z, [code_of(loads_of(order)) for order in ORDERS])

    barrier = pltpu.get_barrier_semaphore()

    @pl.when(chan > 0)
    def _():
        pl.semaphore_signal(barrier, inc=1, device_id=(obs, chan - 1), device_id_type=MESH)

    @pl.when(chan < last)
    def _():
        pl.semaphore_signal(barrier, inc=1, device_id=(obs, chan + 1), device_id_type=MESH)

    smalls = [
        pltpu.make_async_copy(source, target, small_sem.at[n])
        for n, (source, target) in enumerate(
            [
                (pred_hbm, pred_ref),
                (lines_hbm, lines_ref),
                (sel_hbm, sel_ref),
                (ids_hbm, ids_ref),
                (inv_hbm, inv_ref),
            ]
        )
    ]
    for copy in smalls:
        copy.start()

    def load(order):
        number = load_code // 8**order % 8
        at = pl.multiple_of(number * BLOCK, BLOCK)
        return pltpu.make_async_copy(
            dep_ref.at[pl.ds(at, BLOCK)],
            cells.at[pl.ds(pl.multiple_of(at + HALO, HALO), BLOCK)],
            load_sem.at[order],
        )

    for order in range(blocks):
        load(order).start()

    for d in range(1, 8):
        pl.semaphore_signal(barrier, inc=1, device_id=((z + d) % 8 * 8 + p, chan), device_id_type=MESH)
        pl.semaphore_signal(barrier, inc=1, device_id=(z * 8 + (p + d) % 8, chan), device_id_type=MESH)

    @pl.when(chan == 0)
    def _():
        cells[pl.ds(0, HALO), :] = jnp.zeros((HALO, cells.shape[1]), jnp.bfloat16)

    @pl.when(chan == last)
    def _():
        cells[pl.ds(HALO + rows, HALO), :] = jnp.zeros((HALO, cells.shape[1]), jnp.bfloat16)

    for copy in smalls:
        copy.wait()

    here = pl.multiple_of(chan * 16, 16)
    id_rows[pl.ds(8, 16), :] = ids_ref[pl.ds(here, 16), :].astype(jnp.float32)
    before = ids_ref[pl.ds(jnp.maximum(here - 1, 0), 1), :].astype(jnp.float32)
    after = ids_ref[pl.ds(jnp.minimum(here + 16, 16 * last + 15), 1), :].astype(jnp.float32)
    id_rows[pl.ds(7, 1), :] = jnp.where(chan > 0, before, -1.0)
    id_rows[pl.ds(24, 1), :] = jnp.where(chan < last, after, -1.0)
    lane16 = lax.broadcasted_iota(jnp.int32, (16, 128), 1)
    turned = [pltpu.roll(id_rows[pl.ds(7 + n, 16), :], 32, axis=1) for n in range(3)]
    id_cols[:, 0:128] = jnp.where(lane16 < 32, turned[0], turned[1])
    id_cols[:, 128:256] = jnp.where(lane16 < 32, turned[1], turned[2])

    for s in range(cells.shape[1] // 128):
        lane = lax.broadcasted_iota(jnp.int32, (PRED, 128), 1)
        values = pred_ref[:, s * 128 : s * 128 + 128].astype(jnp.float32)
        values = jnp.where(lane < lines_ref[s], values, 0.0)
        values = jnp.concatenate([values, jnp.zeros((16 - PRED, 128), jnp.float32)], axis=0)
        live_pred[:, s * 128 : s * 128 + 128] = values.astype(jnp.bfloat16)
        picked = jnp.dot(
            values.T.astype(jnp.bfloat16), sel_ref[...], preferred_element_type=jnp.float32
        )
        products = (picked[:, 0:128] * picked[:, 128:256]).astype(jnp.bfloat16)
        wq[pl.ds(s * 128, 128), :] = jnp.concatenate([products, jnp.zeros_like(products)], axis=1)

    def band(first):
        block = first // 128
        entries = inv_ref[:, pl.ds(first, 128)].astype(jnp.float32)
        number = jnp.broadcast_to(id_rows[pl.ds(8 + block, 1), :], (64, 128))
        both = jnp.concatenate([entries, jnp.zeros((1, 128), jnp.float32), number], axis=0).T
        lane = lax.broadcasted_iota(jnp.int32, (128, 128), 1)
        entries = jnp.where(lane < 64, both, 0.0)
        number = jnp.where(lane < 64, pltpu.roll(both, 64, axis=1), both)
        wide = jnp.concatenate([entries, jnp.zeros_like(entries)], axis=1)
        wide = pltpu.roll(wide, 1, axis=1, stride=1, stride_axis=0)
        near = id_cols[pl.ds(block, 1), :]
        same = jnp.concatenate([number, number], axis=1) == near
        return jnp.where(same, wide, 0.0).astype(jnp.bfloat16)

    def start_of(number):
        return pl.multiple_of(number * BLOCK, BLOCK)

    def make(number, mat):
        for n in range(2):
            mat[n] = band(pl.multiple_of(start_of(number) + 128 * n, 128))

    def product(number, mat, part):
        first = start_of(number)
        cols = pl.ds(part * 256, 256)
        return [
            jnp.dot(
                mat[n][:, 0:WINDOW],
                cells[pl.ds(pl.multiple_of(first + 128 * n, 128), WINDOW), cols],
                preferred_element_type=jnp.float32,
            )
            for n in range(2)
        ]

    def weigh(weighted):
        weight = [(1.0 / jnp.maximum(jnp.abs(w), 1.0)).astype(jnp.bfloat16) for w in weighted]
        scaled = [jnp.clip(w, -1.0, 1.0).astype(jnp.bfloat16) for w in weighted]
        return jnp.concatenate(weight, axis=0), jnp.concatenate(scaled, axis=0)

    for order in range(3):
        load(order).wait()
    make(order_code % 8, mat_a)
    weight0[...], scaled0[...] = weigh(product(order_code % 8, mat_a, 0))

    pl.semaphore_wait(barrier, 14 + jnp.minimum(chan, 1) + jnp.minimum(last - chan, 1))

    def up():
        return pltpu.make_async_remote_copy(
            src_ref=dep_ref.at[pl.ds(0, HALO)],
            dst_ref=cells.at[pl.ds(HALO + rows, HALO)],
            send_sem=halo_send.at[0],
            recv_sem=halo_recv.at[0],
            device_id=(obs, jnp.maximum(chan - 1, 0)),
            device_id_type=MESH,
        )

    def down():
        return pltpu.make_async_remote_copy(
            src_ref=dep_ref.at[pl.ds(rows - HALO, HALO)],
            dst_ref=cells.at[pl.ds(0, HALO)],
            send_sem=halo_send.at[1],
            recv_sem=halo_recv.at[1],
            device_id=(obs, jnp.minimum(chan + 1, last)),
            device_id_type=MESH,
        )

    @pl.when(chan > 0)
    def _():
        up().start()

    @pl.when(chan < last)
    def _():
        down().start()

    def to_plane(number):
        return pltpu.make_async_remote_copy(
            src_ref=send1.at[number],
            dst_ref=recv1.at[z],
            send_sem=send1_sem,
            recv_sem=recv1_sem,
            device_id=(number * 8 + p, chan),
            device_id_type=MESH,
        )

    def block_step(step, number, following, mat, mat_next):

        for start in range(2):

            @pl.when(step == start)
            def _(start=start):
                for order in range(3 + 3 * start, min(6 + 3 * start, blocks)):
                    load(order).wait()

        @pl.when((following == 0) & (chan > 0))
        def _():
            down().wait_recv()

        @pl.when((following == blocks - 1) & (chan < last))
        def _():
            up().wait_recv()

        make(following, mat_next)
        total = jnp.zeros((BLOCK, 256), jnp.float32)
        sides = jnp.zeros((16, BLOCK), jnp.float32)
        weight, scaled = weight0[...], scaled0[...]
        for part in range(parts):
            if part < parts - 1:
                coming = product(number, mat, part + 1)
            else:
                coming = product(following, mat_next, 0)
            cols = pl.ds(part * 256, 256)
            total = total + jnp.dot(weight, wq[cols, :], preferred_element_type=jnp.float32)
            sides = sides + lax.dot_general(
                live_pred[:, cols], scaled, (((1,), (1,)), ((), ())), preferred_element_type=jnp.float32
            )
            weight, scaled = weigh(coming)
        weight0[...], scaled0[...] = weight, scaled

        lane = lax.broadcasted_iota(jnp.int32, (8, 16, 128), 2)
        halves = total[:, 0:128].reshape(8, 2, 16, 128)
        main = jnp.where(lane < HALF, halves[:, 0], halves[:, 1]).reshape(16, 8, 128)
        own[0:16] = main
        send1[number, 0:16] = main.astype(jnp.bfloat16)
        rest = jnp.concatenate([sides[8:10, 0:128], sides[8:10, 128:256], jnp.zeros((4, 128), jnp.float32)], axis=0)
        for n, tile in enumerate((sides[0:8, 0:128], sides[0:8, 128:256], rest)):
            own[16 + n] = tile
            send1[number, 16 + n] = tile.astype(jnp.bfloat16)

        @pl.when(step < blocks - 1)
        def _():
            to_plane(number).start()

    def pair(n, code):
        first, second, third = code % 8, code // 8 % 8, code // 64 % 8
        block_step(2 * n, first, second, mat_a, mat_b)
        block_step(2 * n + 1, second, third, mat_b, mat_a)
        return code // 64

    lax.fori_loop(0, blocks // 2, pair, order_code)

    def wait_for(buffer, sem):
        pltpu.make_async_copy(buffer.at[pl.ds(0, 7)], buffer.at[pl.ds(0, 7)], sem).wait()

    wait_for(recv1, recv1_sem)
    sums = own[...]
    for source in range(8):
        came = recv1[source].astype(jnp.float32)
        sums = sums + jnp.where(source == z, jnp.zeros_like(came), came)
    for peer in range(8):
        send2[peer, 0:2] = sums[2 * peer : 2 * peer + 2]
        at = peer % 4 * 32
        low, high = sums[16 + peer // 4][:, at : at + 32], sums[18][:, at : at + 32]
        send2[peer, 2] = jnp.concatenate([low, high, jnp.zeros((8, 64), jnp.float32)], axis=1)

    @pl.loop(1, 8)
    def _(d):
        peer = (p + d) % 8
        pltpu.make_async_remote_copy(
            src_ref=send2.at[peer],
            dst_ref=recv2.at[p],
            send_sem=send2_sem,
            recv_sem=recv2_sem,
            device_id=(z * 8 + peer, chan),
            device_id_type=MESH,
        ).start()

    mine = send2[p]
    wait_for(recv2, recv2_sem)
    whole = mine
    for source in range(8):
        came = recv2[source]
        whole = whole + jnp.where(source == p, jnp.zeros_like(came), came)
    whole = whole * factor
    flat = whole[0:2].reshape(16, 128).T
    values = jnp.concatenate([flat[0:HALF], flat[HALF:128]], axis=1)
    index = {pair: m for m, pair in enumerate(PAIRS)}
    for j in range(PRED):
        for k in range(PRED):
            m = index[(min(j, k), max(j, k))]
            gram_ref[pl.ds(j * PRED + k, 1), :] = values[m : m + 1, :]
    rhs_ref[0:8, :] = whole[2][:, 0:32]
    rest = whole[2][:, 32:64]
    rhs_ref[8:PRED, :] = jnp.where(p < 4, rest[0:2, :], rest[2:4, :])

    wait_for(send1, send1_sem)
    wait_for(send2, send2_sem)

    @pl.when(chan > 0)
    def _():
        up().wait_send()

    @pl.when(chan < last)
    def _():
        down().wait_send()


def on_device(departures, predictors, inv_band, band_id, line_counts):
    rows, obs_dev = departures.shape
    owned = rows // lax.axis_size("obs")
    vmem = pl.BlockSpec(memory_space=pltpu.VMEM)
    return pl.pallas_call(
        kernel,
        out_shape=(
            jax.ShapeDtypeStruct((PRED * PRED, owned), jnp.float32),
            jax.ShapeDtypeStruct((PRED, owned), jnp.float32),
        ),
        in_specs=[pl.BlockSpec(memory_space=pltpu.HBM)] * 6,
        out_specs=(vmem, vmem),
        scratch_shapes=[
            pltpu.VMEM((rows + 2 * HALO, obs_dev), jnp.bfloat16),
            pltpu.VMEM(predictors.shape, jnp.bfloat16),
            pltpu.VMEM(inv_band.shape, jnp.bfloat16),
            pltpu.VMEM((band_id.shape[0] // 128, 128), jnp.int32),
            pltpu.SMEM(line_counts.shape, jnp.int32),
            pltpu.VMEM((16, 256), jnp.bfloat16),
            pltpu.VMEM((obs_dev, 256), jnp.bfloat16),
            pltpu.VMEM((16, obs_dev), jnp.bfloat16),
            pltpu.VMEM((32, 128), jnp.float32),
            pltpu.VMEM((16, 256), jnp.float32),
            pltpu.VMEM((2, 128, 256), jnp.bfloat16),
            pltpu.VMEM((2, 128, 256), jnp.bfloat16),
            pltpu.VMEM((BLOCK, 256), jnp.bfloat16),
            pltpu.VMEM((BLOCK, 256), jnp.bfloat16),
            pltpu.VMEM((8, TILES, 8, 128), jnp.bfloat16),
            pltpu.VMEM((8, TILES, 8, 128), jnp.bfloat16),
            pltpu.VMEM((TILES, 8, 128), jnp.float32),
            pltpu.VMEM((8, 3, 8, 128), jnp.float32),
            pltpu.VMEM((8, 3, 8, 128), jnp.float32),
            pltpu.SemaphoreType.DMA((5,)),
            pltpu.SemaphoreType.DMA((8,)),
            pltpu.SemaphoreType.DMA((2,)),
            pltpu.SemaphoreType.DMA((2,)),
            pltpu.SemaphoreType.DMA,
            pltpu.SemaphoreType.DMA,
            pltpu.SemaphoreType.DMA,
            pltpu.SemaphoreType.DMA,
        ],
        compiler_params=pltpu.CompilerParams(collective_id=0, has_side_effects=True),
        name="normal_equations",
    )(
        departures,
        predictors,
        inv_band,
        band_id.reshape(band_id.shape[0] // 128, 128),
        line_counts,
        jnp.asarray(selectors(), jnp.bfloat16),
    )


def solution(mesh):
    in_specs = (P("chan", "obs"), P(None, "obs"), P(None, "chan"), P(), P("obs"))
    out_specs = (P(None, ("chan", "obs")), P(None, ("chan", "obs")))
    return jax.shard_map(
        on_device, mesh=mesh, in_specs=in_specs, out_specs=out_specs, check_vma=False
    )
```

```python
import functools

import jax
import jax.numpy as jnp
import numpy as np
from jax import lax
from jax.experimental import pallas as pl
from jax.experimental.pallas import tpu as pltpu
from jax.sharding import PartitionSpec as P

MESH = pl.DeviceIdType.MESH
PRED = 10
HALO = 32
BLOCK = 256
WINDOW = 192
PAIRS = [(j, k) for j in range(PRED) for k in range(j, PRED)]
HALF = 64
TILES = 19

ORDERS = (
    (2, 5, 4, 3, 1, 6, 7, 0),
    (5, 2, 3, 6, 4, 0, 7, 1),
    (4, 5, 1, 6, 0, 3, 7, 2),
    (1, 5, 6, 0, 2, 4, 7, 3),
    (6, 1, 2, 0, 5, 3, 7, 4),
    (1, 4, 2, 3, 0, 7, 6, 5),
    (3, 1, 2, 5, 0, 4, 7, 6),
    (2, 5, 1, 3, 4, 0, 6, 7),
)
FAR = (4,)


def loads_of(order):
    needed = []
    for block in order:
        for near in (block - 1, block, block + 1):
            if 0 <= near < len(order) and near not in needed:
                needed.append(near)
    return tuple(needed)


def code_of(order):
    return sum(block * 8**n for n, block in enumerate(order))


def pick(z, codes):
    code = jnp.int32(codes[0])
    for n in range(1, len(codes)):
        code = jnp.where(z == n, jnp.int32(codes[n]), code)
    return code


def selectors():
    left = np.zeros((16, 128), np.float32)
    right = np.zeros((16, 128), np.float32)
    for half in range(2):
        for m, (j, k) in enumerate(PAIRS):
            left[j, half * HALF + m] = 1
            right[k, half * HALF + m] = 1
    return np.concatenate([left, right], axis=1)


def kernel(
    dep_ref, pred_hbm, inv_hbm, ids_hbm, lines_hbm, sel_hbm,
    sum_ref,
    cells, pred_ref, inv_ref, ids_ref, lines_ref, sel_ref,
    wq, live_pred, id_rows, id_cols, mat_a, mat_b, weight0, scaled0,
    send1, recv1, own, send2, recv2, far_send, far_recv, far_own, far_sum,
    small_sem, load_sem, halo_send, halo_recv, send1_sem, recv1_sem, send2_sem, recv2_sem,
    far_send_sem, far_recv_sem,
):
    obs = lax.axis_index("obs")
    chan = lax.axis_index("chan")
    z, p = obs // 8, obs % 8
    rows = dep_ref.shape[0]
    blocks = rows // BLOCK
    parts = cells.shape[1] // 256
    factor = 1.0 / float(dep_ref.shape[1] * lax.axis_size("obs"))
    last = lax.axis_size("chan") - 1
    order_code = pick(z, [code_of(order + order[:1]) for order in ORDERS])
    load_code = pick(z, [code_of(loads_of(order)) for order in ORDERS])

    barrier = pltpu.get_barrier_semaphore()

    @pl.when(chan > 0)
    def _():
        pl.semaphore_signal(barrier, inc=1, device_id=(obs, chan - 1), device_id_type=MESH)

    @pl.when(chan < last)
    def _():
        pl.semaphore_signal(barrier, inc=1, device_id=(obs, chan + 1), device_id_type=MESH)

    smalls = [
        pltpu.make_async_copy(source, target, small_sem.at[n])
        for n, (source, target) in enumerate(
            [
                (pred_hbm, pred_ref),
                (lines_hbm, lines_ref),
                (sel_hbm, sel_ref),
                (ids_hbm, ids_ref),
                (inv_hbm, inv_ref),
            ]
        )
    ]
    for copy in smalls:
        copy.start()

    def load(order):
        number = load_code // 8**order % 8
        at = pl.multiple_of(number * BLOCK, BLOCK)
        return pltpu.make_async_copy(
            dep_ref.at[pl.ds(at, BLOCK)],
            cells.at[pl.ds(pl.multiple_of(at + HALO, HALO), BLOCK)],
            load_sem.at[order],
        )

    for order in range(blocks):
        load(order).start()

    for d in range(1, 8):
        pl.semaphore_signal(barrier, inc=1, device_id=((z + d) % 8 * 8 + p, chan), device_id_type=MESH)
        pl.semaphore_signal(barrier, inc=1, device_id=(z * 8 + (p + d) % 8, chan), device_id_type=MESH)

    @pl.when(chan == 0)
    def _():
        cells[pl.ds(0, HALO), :] = jnp.zeros((HALO, cells.shape[1]), jnp.bfloat16)

    @pl.when(chan == last)
    def _():
        cells[pl.ds(HALO + rows, HALO), :] = jnp.zeros((HALO, cells.shape[1]), jnp.bfloat16)

    for copy in smalls:
        copy.wait()

    here = pl.multiple_of(chan * 16, 16)
    id_rows[pl.ds(8, 16), :] = ids_ref[pl.ds(here, 16), :].astype(jnp.float32)
    before = ids_ref[pl.ds(jnp.maximum(here - 1, 0), 1), :].astype(jnp.float32)
    after = ids_ref[pl.ds(jnp.minimum(here + 16, 16 * last + 15), 1), :].astype(jnp.float32)
    id_rows[pl.ds(7, 1), :] = jnp.where(chan > 0, before, -1.0)
    id_rows[pl.ds(24, 1), :] = jnp.where(chan < last, after, -1.0)
    lane16 = lax.broadcasted_iota(jnp.int32, (16, 128), 1)
    turned = [pltpu.roll(id_rows[pl.ds(7 + n, 16), :], 32, axis=1) for n in range(3)]
    id_cols[:, 0:128] = jnp.where(lane16 < 32, turned[0], turned[1])
    id_cols[:, 128:256] = jnp.where(lane16 < 32, turned[1], turned[2])

    for s in range(cells.shape[1] // 128):
        lane = lax.broadcasted_iota(jnp.int32, (PRED, 128), 1)
        values = pred_ref[:, s * 128 : s * 128 + 128].astype(jnp.float32)
        values = jnp.where(lane < lines_ref[s], values, 0.0)
        values = jnp.concatenate([values, jnp.zeros((16 - PRED, 128), jnp.float32)], axis=0)
        live_pred[:, s * 128 : s * 128 + 128] = values.astype(jnp.bfloat16)
        picked = jnp.dot(
            values.T.astype(jnp.bfloat16), sel_ref[...], preferred_element_type=jnp.float32
        )
        products = (picked[:, 0:128] * picked[:, 128:256]).astype(jnp.bfloat16)
        wq[pl.ds(s * 128, 128), :] = jnp.concatenate([products, jnp.zeros_like(products)], axis=1)

    def band(first):
        block = first // 128
        entries = inv_ref[:, pl.ds(first, 128)].astype(jnp.float32)
        number = jnp.broadcast_to(id_rows[pl.ds(8 + block, 1), :], (64, 128))
        both = jnp.concatenate([entries, jnp.zeros((1, 128), jnp.float32), number], axis=0).T
        lane = lax.broadcasted_iota(jnp.int32, (128, 128), 1)
        entries = jnp.where(lane < 64, both, 0.0)
        number = jnp.where(lane < 64, pltpu.roll(both, 64, axis=1), both)
        wide = jnp.concatenate([entries, jnp.zeros_like(entries)], axis=1)
        wide = pltpu.roll(wide, 1, axis=1, stride=1, stride_axis=0)
        near = id_cols[pl.ds(block, 1), :]
        same = jnp.concatenate([number, number], axis=1) == near
        return jnp.where(same, wide, 0.0).astype(jnp.bfloat16)

    def start_of(number):
        return pl.multiple_of(number * BLOCK, BLOCK)

    def make(number, mat):
        for n in range(2):
            mat[n] = band(pl.multiple_of(start_of(number) + 128 * n, 128))

    def product(number, mat, part):
        first = start_of(number)
        cols = pl.ds(part * 256, 256)
        return [
            jnp.dot(
                mat[n][:, 0:WINDOW],
                cells[pl.ds(pl.multiple_of(first + 128 * n, 128), WINDOW), cols],
                preferred_element_type=jnp.float32,
            )
            for n in range(2)
        ]

    def weigh(weighted):
        weight = [(1.0 / jnp.maximum(jnp.abs(w), 1.0)).astype(jnp.bfloat16) for w in weighted]
        scaled = [jnp.clip(w, -1.0, 1.0).astype(jnp.bfloat16) for w in weighted]
        return jnp.concatenate(weight, axis=0), jnp.concatenate(scaled, axis=0)

    for order in range(3):
        load(order).wait()
    make(order_code % 8, mat_a)
    weight0[...], scaled0[...] = weigh(product(order_code % 8, mat_a, 0))

    pl.semaphore_wait(barrier, 14 + jnp.minimum(chan, 1) + jnp.minimum(last - chan, 1))

    def up():
        return pltpu.make_async_remote_copy(
            src_ref=dep_ref.at[pl.ds(0, HALO)],
            dst_ref=cells.at[pl.ds(HALO + rows, HALO)],
            send_sem=halo_send.at[0],
            recv_sem=halo_recv.at[0],
            device_id=(obs, jnp.maximum(chan - 1, 0)),
            device_id_type=MESH,
        )

    def down():
        return pltpu.make_async_remote_copy(
            src_ref=dep_ref.at[pl.ds(rows - HALO, HALO)],
            dst_ref=cells.at[pl.ds(0, HALO)],
            send_sem=halo_send.at[1],
            recv_sem=halo_recv.at[1],
            device_id=(obs, jnp.minimum(chan + 1, last)),
            device_id_type=MESH,
        )

    @pl.when(chan > 0)
    def _():
        up().start()

    @pl.when(chan < last)
    def _():
        down().start()

    def to_plane(number):
        return pltpu.make_async_remote_copy(
            src_ref=send1.at[number],
            dst_ref=recv1.at[z],
            send_sem=send1_sem,
            recv_sem=recv1_sem,
            device_id=(number * 8 + p, chan),
            device_id_type=MESH,
        )

    def split(tiles, target):
        for peer in range(8):
            target[peer, 0:2] = tiles[2 * peer : 2 * peer + 2]
            at = peer % 4 * 32
            low, high = tiles[16 + peer // 4][:, at : at + 32], tiles[18][:, at : at + 32]
            target[peer, 2] = jnp.concatenate([low, high, jnp.zeros((8, 64), jnp.float32)], axis=1)

    def block_step(step, number, following, mat, mat_next):

        for start in range(2):

            @pl.when(step == start)
            def _(start=start):
                for order in range(3 + 3 * start, min(6 + 3 * start, blocks)):
                    load(order).wait()

        @pl.when((following == 0) & (chan > 0))
        def _():
            down().wait_recv()

        @pl.when((following == blocks - 1) & (chan < last))
        def _():
            up().wait_recv()

        make(following, mat_next)
        total = jnp.zeros((BLOCK, 256), jnp.float32)
        sides = jnp.zeros((16, BLOCK), jnp.float32)
        weight, scaled = weight0[...], scaled0[...]
        for part in range(parts):
            if part < parts - 1:
                coming = product(number, mat, part + 1)
            else:
                coming = product(following, mat_next, 0)
            cols = pl.ds(part * 256, 256)
            total = total + jnp.dot(weight, wq[cols, :], preferred_element_type=jnp.float32)
            sides = sides + lax.dot_general(
                live_pred[:, cols], scaled, (((1,), (1,)), ((), ())), preferred_element_type=jnp.float32
            )
            weight, scaled = weigh(coming)
        weight0[...], scaled0[...] = weight, scaled

        lane = lax.broadcasted_iota(jnp.int32, (8, 16, 128), 2)
        halves = total[:, 0:128].reshape(8, 2, 16, 128)
        main = jnp.where(lane < HALF, halves[:, 0], halves[:, 1]).reshape(16, 8, 128)
        own[0:16] = main
        send1[number, 0:16] = main.astype(jnp.bfloat16)
        rest = jnp.concatenate([sides[8:10, 0:128], sides[8:10, 128:256], jnp.zeros((4, 128), jnp.float32)], axis=0)
        for n, tile in enumerate((sides[0:8, 0:128], sides[0:8, 128:256], rest)):
            own[16 + n] = tile
            send1[number, 16 + n] = tile.astype(jnp.bfloat16)

        ahead = (number - z + blocks) % blocks
        near = ahead > 0
        for n, distance in enumerate(FAR):
            near = near & (ahead != distance)

            @pl.when(ahead == distance)
            def _(n=n):
                split(own[...], send2)
                far_send[n] = send2[...].astype(jnp.bfloat16)
                far_own[n] = send2[p]

                @pl.loop(1, 8)
                def _(d):
                    peer = (p + d) % 8
                    pltpu.make_async_remote_copy(
                        src_ref=far_send.at[n, peer],
                        dst_ref=far_recv.at[n, p],
                        send_sem=far_send_sem.at[n],
                        recv_sem=far_recv_sem.at[n],
                        device_id=(z * 8 + peer, chan),
                        device_id_type=MESH,
                    ).start()

        @pl.when(near)
        def _():
            to_plane(number).start()

    def pair(n, code):
        first, second, third = code % 8, code // 8 % 8, code // 64 % 8
        block_step(2 * n, first, second, mat_a, mat_b)
        block_step(2 * n + 1, second, third, mat_b, mat_a)
        return code // 64

    lax.fori_loop(0, blocks // 2, pair, order_code)

    def wait_for(buffer, count, sem):
        pltpu.make_async_copy(buffer.at[pl.ds(0, count)], buffer.at[pl.ds(0, count)], sem).wait()

    def far_copy(n):
        return pltpu.make_async_remote_copy(
            src_ref=far_sum.at[n],
            dst_ref=recv2.at[8 + n],
            send_sem=send2_sem,
            recv_sem=recv2_sem,
            device_id=((z + FAR[n]) % 8 * 8 + p, chan),
            device_id_type=MESH,
        )

    for n in range(len(FAR)):
        wait_for(far_recv.at[n], 7, far_recv_sem.at[n])
        chunk = far_own[n]
        for source in range(8):
            came = far_recv[n, source].astype(jnp.float32)
            chunk = chunk + jnp.where(source == p, jnp.zeros_like(came), came)
        far_sum[n] = chunk
        far_copy(n).start()

    wait_for(recv1, 7 - len(FAR), recv1_sem)
    sums = own[...]
    for source in range(8):
        came = recv1[source].astype(jnp.float32)
        away = (z - source + 8) % 8
        absent = away == 0
        for distance in FAR:
            absent = absent | (away == distance)
        sums = sums + jnp.where(absent, jnp.zeros_like(came), came)
    split(sums, send2)

    @pl.loop(1, 8)
    def _(d):
        peer = (p + d) % 8
        pltpu.make_async_remote_copy(
            src_ref=send2.at[peer],
            dst_ref=recv2.at[p],
            send_sem=send2_sem,
            recv_sem=recv2_sem,
            device_id=(z * 8 + peer, chan),
            device_id_type=MESH,
        ).start()

    mine = send2[p]
    wait_for(recv2, 7 + len(FAR), recv2_sem)
    whole = mine
    for source in range(8):
        came = recv2[source]
        whole = whole + jnp.where(source == p, jnp.zeros_like(came), came)
    for n in range(len(FAR)):
        whole = whole + recv2[8 + n]
    rest = whole[2]
    lane = lax.broadcasted_iota(jnp.int32, (8, 128), 1)
    row = lax.broadcasted_iota(jnp.int32, (8, 128), 0)
    moved = pltpu.roll(rest, 6, axis=0)
    sum_ref[0:2] = whole[0:2] * factor
    sum_ref[2] = jnp.where((lane >= 32) & (row < 2) & (p >= 4), moved, rest) * factor

    wait_for(send1, 7 - len(FAR), send1_sem)
    wait_for(recv2, 7 + len(FAR), send2_sem)
    for n in range(len(FAR)):
        wait_for(far_send.at[n], 7, far_send_sem.at[n])

    @pl.when(chan > 0)
    def _():
        up().wait_send()

    @pl.when(chan < last)
    def _():
        down().wait_send()


def unpack(sum_ref, gram_ref, rhs_ref):
    pairs = sum_ref[0:2].reshape(16, 128)
    pairs = jnp.concatenate([pairs, pltpu.roll(pairs, HALF, axis=1)], axis=0)
    entry = lax.broadcasted_iota(jnp.int32, (32, 128), 1)
    left = jnp.zeros_like(entry)
    for n in range(1, PRED):
        left = left + jnp.where(entry >= n * PRED, 1, 0)
    right = entry - left * PRED
    low, high = jnp.minimum(left, right), jnp.maximum(left, right)
    column = jnp.where(entry < PRED * PRED, low * PRED - (low * (low + 1)) // 2 + high, 0)
    spread = jnp.take_along_axis(pairs, column, axis=1, mode="promise_in_bounds")
    gram_ref[...] = spread[:, 0 : PRED * PRED]
    rhs_ref[0:8, :] = sum_ref[2][:, 0:32]
    rhs_ref[8:PRED, :] = sum_ref[2][0 : PRED - 8, 32:64]


def on_device(departures, predictors, inv_band, band_id, line_counts):
    rows, obs_dev = departures.shape
    owned = rows // lax.axis_size("obs")
    vmem = pl.BlockSpec(memory_space=pltpu.VMEM)
    sums = pl.pallas_call(
        kernel,
        out_shape=pltpu.VMEM((3, 8, 128), jnp.float32),
        in_specs=[pl.BlockSpec(memory_space=pltpu.HBM)] * 6,
        out_specs=vmem,
        scratch_shapes=[
            pltpu.VMEM((rows + 2 * HALO, obs_dev), jnp.bfloat16),
            pltpu.VMEM(predictors.shape, jnp.bfloat16),
            pltpu.VMEM(inv_band.shape, jnp.bfloat16),
            pltpu.VMEM((band_id.shape[0] // 128, 128), jnp.int32),
            pltpu.SMEM(line_counts.shape, jnp.int32),
            pltpu.VMEM((16, 256), jnp.bfloat16),
            pltpu.VMEM((obs_dev, 256), jnp.bfloat16),
            pltpu.VMEM((16, obs_dev), jnp.bfloat16),
            pltpu.VMEM((32, 128), jnp.float32),
            pltpu.VMEM((16, 256), jnp.float32),
            pltpu.VMEM((2, 128, 256), jnp.bfloat16),
            pltpu.VMEM((2, 128, 256), jnp.bfloat16),
            pltpu.VMEM((BLOCK, 256), jnp.bfloat16),
            pltpu.VMEM((BLOCK, 256), jnp.bfloat16),
            pltpu.VMEM((8, TILES, 8, 128), jnp.bfloat16),
            pltpu.VMEM((8, TILES, 8, 128), jnp.bfloat16),
            pltpu.VMEM((TILES, 8, 128), jnp.float32),
            pltpu.VMEM((8, 3, 8, 128), jnp.float32),
            pltpu.VMEM((8 + len(FAR), 3, 8, 128), jnp.float32),
            pltpu.VMEM((len(FAR), 8, 3, 8, 128), jnp.bfloat16),
            pltpu.VMEM((len(FAR), 8, 3, 8, 128), jnp.bfloat16),
            pltpu.VMEM((len(FAR), 3, 8, 128), jnp.float32),
            pltpu.VMEM((len(FAR), 3, 8, 128), jnp.float32),
            pltpu.SemaphoreType.DMA((5,)),
            pltpu.SemaphoreType.DMA((8,)),
            pltpu.SemaphoreType.DMA((2,)),
            pltpu.SemaphoreType.DMA((2,)),
            pltpu.SemaphoreType.DMA,
            pltpu.SemaphoreType.DMA,
            pltpu.SemaphoreType.DMA,
            pltpu.SemaphoreType.DMA,
            pltpu.SemaphoreType.DMA((len(FAR),)),
            pltpu.SemaphoreType.DMA((len(FAR),)),
        ],
        compiler_params=pltpu.CompilerParams(collective_id=0, has_side_effects=True),
        name="normal_equations",
    )(
        departures,
        predictors,
        inv_band,
        band_id.reshape(band_id.shape[0] // 128, 128),
        line_counts,
        jnp.asarray(selectors(), jnp.bfloat16),
    )
    gram, rhs = pl.pallas_call(
        unpack,
        out_shape=(
            jax.ShapeDtypeStruct((owned, PRED * PRED), jnp.float32),
            jax.ShapeDtypeStruct((PRED, owned), jnp.float32),
        ),
        in_specs=[vmem],
        out_specs=(vmem, vmem),
        name="unpack",
    )(sums)
    return gram.T, rhs


def solution(mesh):
    in_specs = (P("chan", "obs"), P(None, "obs"), P(None, "chan"), P(), P("obs"))
    out_specs = (P(None, ("chan", "obs")), P(None, ("chan", "obs")))
    return jax.shard_map(
        on_device, mesh=mesh, in_specs=in_specs, out_specs=out_specs, check_vma=False
    )
```

```python
import functools

import jax
import jax.numpy as jnp
import numpy as np
from jax import lax
from jax.experimental import pallas as pl
from jax.experimental.pallas import tpu as pltpu
from jax.sharding import PartitionSpec as P

MESH = pl.DeviceIdType.MESH
PRED = 10
HALO = 32
BLOCK = 256
WINDOW = 192
PAIRS = [(j, k) for j in range(PRED) for k in range(j, PRED)]
HALF = 64
TILES = 19

ORDERS = (
    (2, 5, 4, 3, 1, 6, 7, 0),
    (5, 2, 3, 6, 4, 0, 7, 1),
    (4, 5, 1, 6, 0, 3, 7, 2),
    (1, 5, 6, 0, 2, 4, 7, 3),
    (6, 1, 2, 0, 5, 3, 7, 4),
    (1, 4, 2, 3, 0, 7, 6, 5),
    (3, 1, 2, 5, 0, 4, 7, 6),
    (2, 5, 1, 3, 4, 0, 6, 7),
)
FAR = (4,)


def loads_of(order):
    needed = []
    for block in order:
        for near in (block - 1, block, block + 1):
            if 0 <= near < len(order) and near not in needed:
                needed.append(near)
    return tuple(needed)


def code_of(order):
    return sum(block * 8**n for n, block in enumerate(order))


def pick(z, codes):
    code = jnp.int32(codes[0])
    for n in range(1, len(codes)):
        code = jnp.where(z == n, jnp.int32(codes[n]), code)
    return code


def selectors():
    left = np.zeros((16, 128), np.float32)
    right = np.zeros((16, 128), np.float32)
    for half in range(2):
        for m, (j, k) in enumerate(PAIRS):
            left[j, half * HALF + m] = 1
            right[k, half * HALF + m] = 1
    return np.concatenate([left, right], axis=1)


def kernel(
    dep_ref, pred_hbm, inv_hbm, ids_hbm, lines_hbm, sel_hbm,
    sum_ref,
    cells, edges, pred_ref, inv_ref, ids_ref, lines_ref, sel_ref,
    wq, live_pred, id_rows, id_cols, mat_a, mat_b, weight0, scaled0,
    send1, recv1, own, send2, recv2, far_send, far_recv, far_own, far_sum,
    small_sem, load_sem, edge_sem, halo_send, halo_recv, send1_sem, recv1_sem, send2_sem, recv2_sem,
    far_send_sem, far_recv_sem,
):
    smalls = [
        pltpu.make_async_copy(source, target, small_sem.at[n])
        for n, (source, target) in enumerate(
            [
                (pred_hbm, pred_ref),
                (lines_hbm, lines_ref),
                (sel_hbm, sel_ref),
                (ids_hbm, ids_ref),
                (inv_hbm, inv_ref),
            ]
        )
    ]
    for copy in smalls:
        copy.start()

    obs = lax.axis_index("obs")
    chan = lax.axis_index("chan")
    z, p = obs // 8, obs % 8
    rows = dep_ref.shape[0]
    blocks = rows // BLOCK
    parts = cells.shape[1] // 256
    factor = 1.0 / float(dep_ref.shape[1] * lax.axis_size("obs"))
    last = lax.axis_size("chan") - 1
    order_code = pick(z, [code_of(order + order[:1]) for order in ORDERS])
    load_code = pick(z, [code_of(loads_of(order)) for order in ORDERS])

    barrier = pltpu.get_barrier_semaphore()

    @pl.when(chan > 0)
    def _():
        pl.semaphore_signal(barrier, inc=1, device_id=(obs, chan - 1), device_id_type=MESH)

    @pl.when(chan < last)
    def _():
        pl.semaphore_signal(barrier, inc=1, device_id=(obs, chan + 1), device_id_type=MESH)

    def load(order):
        number = load_code // 8**order % 8
        at = pl.multiple_of(number * BLOCK, BLOCK)
        return pltpu.make_async_copy(
            dep_ref.at[pl.ds(at, BLOCK)],
            cells.at[pl.ds(pl.multiple_of(at + HALO, HALO), BLOCK)],
            load_sem.at[order],
        )

    def edge(n):
        return pltpu.make_async_copy(
            dep_ref.at[pl.ds(n * (rows - HALO), HALO)], edges.at[n], edge_sem.at[n]
        )

    for order in range(blocks):
        load(order).start()
        if order == 2:
            for n in range(2):
                edge(n).start()

    for d in range(1, 8):
        pl.semaphore_signal(barrier, inc=1, device_id=((z + d) % 8 * 8 + p, chan), device_id_type=MESH)
        pl.semaphore_signal(barrier, inc=1, device_id=(z * 8 + (p + d) % 8, chan), device_id_type=MESH)

    @pl.when(chan == 0)
    def _():
        cells[pl.ds(0, HALO), :] = jnp.zeros((HALO, cells.shape[1]), jnp.bfloat16)

    @pl.when(chan == last)
    def _():
        cells[pl.ds(HALO + rows, HALO), :] = jnp.zeros((HALO, cells.shape[1]), jnp.bfloat16)

    for copy in smalls:
        copy.wait()

    here = pl.multiple_of(chan * 16, 16)
    id_rows[pl.ds(8, 16), :] = ids_ref[pl.ds(here, 16), :].astype(jnp.float32)
    before = ids_ref[pl.ds(jnp.maximum(here - 1, 0), 1), :].astype(jnp.float32)
    after = ids_ref[pl.ds(jnp.minimum(here + 16, 16 * last + 15), 1), :].astype(jnp.float32)
    id_rows[pl.ds(7, 1), :] = jnp.where(chan > 0, before, -1.0)
    id_rows[pl.ds(24, 1), :] = jnp.where(chan < last, after, -1.0)
    lane16 = lax.broadcasted_iota(jnp.int32, (16, 128), 1)
    turned = [pltpu.roll(id_rows[pl.ds(7 + n, 16), :], 32, axis=1) for n in range(3)]
    id_cols[:, 0:128] = jnp.where(lane16 < 32, turned[0], turned[1])
    id_cols[:, 128:256] = jnp.where(lane16 < 32, turned[1], turned[2])

    def band(first):
        block = first // 128
        entries = inv_ref[:, pl.ds(first, 128)].astype(jnp.float32)
        number = jnp.broadcast_to(id_rows[pl.ds(8 + block, 1), :], (64, 128))
        both = jnp.concatenate([entries, jnp.zeros((1, 128), jnp.float32), number], axis=0).T
        lane = lax.broadcasted_iota(jnp.int32, (128, 128), 1)
        entries = jnp.where(lane < 64, both, 0.0)
        number = jnp.where(lane < 64, pltpu.roll(both, 64, axis=1), both)
        wide = jnp.concatenate([entries, jnp.zeros_like(entries)], axis=1)
        wide = pltpu.roll(wide, 1, axis=1, stride=1, stride_axis=0)
        near = id_cols[pl.ds(block, 1), :]
        same = jnp.concatenate([number, number], axis=1) == near
        return jnp.where(same, wide, 0.0).astype(jnp.bfloat16)

    def start_of(number):
        return pl.multiple_of(number * BLOCK, BLOCK)

    def make(number, mat):
        for n in range(2):
            mat[n] = band(pl.multiple_of(start_of(number) + 128 * n, 128))

    make(order_code % 8, mat_a)

    for s in range(cells.shape[1] // 128):
        lane = lax.broadcasted_iota(jnp.int32, (PRED, 128), 1)
        values = pred_ref[:, s * 128 : s * 128 + 128].astype(jnp.float32)
        values = jnp.where(lane < lines_ref[s], values, 0.0)
        values = jnp.concatenate([values, jnp.zeros((16 - PRED, 128), jnp.float32)], axis=0)
        live_pred[:, s * 128 : s * 128 + 128] = values.astype(jnp.bfloat16)
        picked = jnp.dot(
            values.T.astype(jnp.bfloat16), sel_ref[...], preferred_element_type=jnp.float32
        )
        products = (picked[:, 0:128] * picked[:, 128:256]).astype(jnp.bfloat16)
        wq[pl.ds(s * 128, 128), :] = jnp.concatenate([products, jnp.zeros_like(products)], axis=1)

    def product(number, mat, part):
        first = start_of(number)
        cols = pl.ds(part * 256, 256)
        return [
            jnp.dot(
                mat[n][:, 0:WINDOW],
                cells[pl.ds(pl.multiple_of(first + 128 * n, 128), WINDOW), cols],
                preferred_element_type=jnp.float32,
            )
            for n in range(2)
        ]

    def weigh(weighted):
        weight = [(1.0 / jnp.maximum(jnp.abs(w), 1.0)).astype(jnp.bfloat16) for w in weighted]
        scaled = [jnp.clip(w, -1.0, 1.0).astype(jnp.bfloat16) for w in weighted]
        return jnp.concatenate(weight, axis=0), jnp.concatenate(scaled, axis=0)

    for order in range(3):
        load(order).wait()
    weight0[...], scaled0[...] = weigh(product(order_code % 8, mat_a, 0))

    pl.semaphore_wait(barrier, 14 + jnp.minimum(chan, 1) + jnp.minimum(last - chan, 1))

    def up():
        return pltpu.make_async_remote_copy(
            src_ref=edges.at[0],
            dst_ref=cells.at[pl.ds(HALO + rows, HALO)],
            send_sem=halo_send.at[0],
            recv_sem=halo_recv.at[0],
            device_id=(obs, jnp.maximum(chan - 1, 0)),
            device_id_type=MESH,
        )

    def down():
        return pltpu.make_async_remote_copy(
            src_ref=edges.at[1],
            dst_ref=cells.at[pl.ds(0, HALO)],
            send_sem=halo_send.at[1],
            recv_sem=halo_recv.at[1],
            device_id=(obs, jnp.minimum(chan + 1, last)),
            device_id_type=MESH,
        )

    for n in range(2):
        edge(n).wait()

    @pl.when(chan > 0)
    def _():
        up().start()

    @pl.when(chan < last)
    def _():
        down().start()

    def to_plane(number):
        return pltpu.make_async_remote_copy(
            src_ref=send1.at[number],
            dst_ref=recv1.at[z],
            send_sem=send1_sem,
            recv_sem=recv1_sem,
            device_id=(number * 8 + p, chan),
            device_id_type=MESH,
        )

    def split(tiles, target):
        for peer in range(8):
            target[peer, 0:2] = tiles[2 * peer : 2 * peer + 2]
            at = peer % 4 * 32
            low, high = tiles[16 + peer // 4][:, at : at + 32], tiles[18][:, at : at + 32]
            target[peer, 2] = jnp.concatenate([low, high, jnp.zeros((8, 64), jnp.float32)], axis=1)

    def block_step(step, number, following, mat, mat_next):

        for start in range(2):

            @pl.when(step == start)
            def _(start=start):
                for order in range(3 + 3 * start, min(6 + 3 * start, blocks)):
                    load(order).wait()

        @pl.when((following == 0) & (chan > 0))
        def _():
            down().wait_recv()

        @pl.when((following == blocks - 1) & (chan < last))
        def _():
            up().wait_recv()

        make(following, mat_next)
        total = jnp.zeros((BLOCK, 256), jnp.float32)
        sides = jnp.zeros((16, BLOCK), jnp.float32)
        weight, scaled = weight0[...], scaled0[...]
        for part in range(parts):
            if part < parts - 1:
                coming = product(number, mat, part + 1)
            else:
                coming = product(following, mat_next, 0)
            cols = pl.ds(part * 256, 256)
            total = total + jnp.dot(weight, wq[cols, :], preferred_element_type=jnp.float32)
            sides = sides + lax.dot_general(
                live_pred[:, cols], scaled, (((1,), (1,)), ((), ())), preferred_element_type=jnp.float32
            )
            weight, scaled = weigh(coming)
        weight0[...], scaled0[...] = weight, scaled

        lane = lax.broadcasted_iota(jnp.int32, (8, 16, 128), 2)
        halves = total[:, 0:128].reshape(8, 2, 16, 128)
        main = jnp.where(lane < HALF, halves[:, 0], halves[:, 1]).reshape(16, 8, 128)
        own[0:16] = main
        send1[number, 0:16] = main.astype(jnp.bfloat16)
        rest = jnp.concatenate([sides[8:10, 0:128], sides[8:10, 128:256], jnp.zeros((4, 128), jnp.float32)], axis=0)
        for n, tile in enumerate((sides[0:8, 0:128], sides[0:8, 128:256], rest)):
            own[16 + n] = tile
            send1[number, 16 + n] = tile.astype(jnp.bfloat16)

        ahead = (number - z + blocks) % blocks
        near = ahead > 0
        for n, distance in enumerate(FAR):
            near = near & (ahead != distance)

            @pl.when(ahead == distance)
            def _(n=n):
                split(own[...], send2)
                far_send[n] = send2[...].astype(jnp.bfloat16)
                far_own[n] = send2[p]

                @pl.loop(1, 8)
                def _(d):
                    peer = (p + d) % 8
                    pltpu.make_async_remote_copy(
                        src_ref=far_send.at[n, peer],
                        dst_ref=far_recv.at[n, p],
                        send_sem=far_send_sem.at[n],
                        recv_sem=far_recv_sem.at[n],
                        device_id=(z * 8 + peer, chan),
                        device_id_type=MESH,
                    ).start()

        @pl.when(near)
        def _():
            to_plane(number).start()

    def pair(n, code):
        first, second, third = code % 8, code // 8 % 8, code // 64 % 8
        block_step(2 * n, first, second, mat_a, mat_b)
        block_step(2 * n + 1, second, third, mat_b, mat_a)
        return code // 64

    lax.fori_loop(0, blocks // 2, pair, order_code)

    def wait_for(buffer, count, sem):
        pltpu.make_async_copy(buffer.at[pl.ds(0, count)], buffer.at[pl.ds(0, count)], sem).wait()

    def far_copy(n):
        return pltpu.make_async_remote_copy(
            src_ref=far_sum.at[n],
            dst_ref=recv2.at[8 + n],
            send_sem=send2_sem,
            recv_sem=recv2_sem,
            device_id=((z + FAR[n]) % 8 * 8 + p, chan),
            device_id_type=MESH,
        )

    for n in range(len(FAR)):
        wait_for(far_recv.at[n], 7, far_recv_sem.at[n])
        chunk = far_own[n]
        for source in range(8):
            came = far_recv[n, source].astype(jnp.float32)
            chunk = chunk + jnp.where(source == p, jnp.zeros_like(came), came)
        far_sum[n] = chunk
        far_copy(n).start()

    wait_for(recv1, 7 - len(FAR), recv1_sem)
    sums = own[...]
    for source in range(8):
        came = recv1[source].astype(jnp.float32)
        away = (z - source + 8) % 8
        absent = away == 0
        for distance in FAR:
            absent = absent | (away == distance)
        sums = sums + jnp.where(absent, jnp.zeros_like(came), came)
    split(sums, send2)

    @pl.loop(1, 8)
    def _(d):
        peer = (p + d) % 8
        pltpu.make_async_remote_copy(
            src_ref=send2.at[peer],
            dst_ref=recv2.at[p],
            send_sem=send2_sem,
            recv_sem=recv2_sem,
            device_id=(z * 8 + peer, chan),
            device_id_type=MESH,
        ).start()

    mine = send2[p]
    wait_for(recv2, 7 + len(FAR), recv2_sem)
    whole = mine
    for source in range(8):
        came = recv2[source]
        whole = whole + jnp.where(source == p, jnp.zeros_like(came), came)
    for n in range(len(FAR)):
        whole = whole + recv2[8 + n]
    rest = whole[2]
    lane = lax.broadcasted_iota(jnp.int32, (8, 128), 1)
    row = lax.broadcasted_iota(jnp.int32, (8, 128), 0)
    moved = pltpu.roll(rest, 6, axis=0)
    sum_ref[0:2] = whole[0:2] * factor
    sum_ref[2] = jnp.where((lane >= 32) & (row < 2) & (p >= 4), moved, rest) * factor

    wait_for(send1, 7 - len(FAR), send1_sem)
    wait_for(recv2, 7 + len(FAR), send2_sem)
    for n in range(len(FAR)):
        wait_for(far_send.at[n], 7, far_send_sem.at[n])

    @pl.when(chan > 0)
    def _():
        up().wait_send()

    @pl.when(chan < last)
    def _():
        down().wait_send()


def unpack(sum_ref, gram_ref, rhs_ref):
    pairs = sum_ref[0:2].reshape(16, 128)
    pairs = jnp.concatenate([pairs, pltpu.roll(pairs, HALF, axis=1)], axis=0)
    entry = lax.broadcasted_iota(jnp.int32, (32, 128), 1)
    left = jnp.zeros_like(entry)
    for n in range(1, PRED):
        left = left + jnp.where(entry >= n * PRED, 1, 0)
    right = entry - left * PRED
    low, high = jnp.minimum(left, right), jnp.maximum(left, right)
    column = jnp.where(entry < PRED * PRED, low * PRED - (low * (low + 1)) // 2 + high, 0)
    spread = jnp.take_along_axis(pairs, column, axis=1, mode="promise_in_bounds")
    gram_ref[...] = spread[:, 0 : PRED * PRED]
    rhs_ref[0:8, :] = sum_ref[2][:, 0:32]
    rhs_ref[8:PRED, :] = sum_ref[2][0 : PRED - 8, 32:64]


def on_device(departures, predictors, inv_band, band_id, line_counts):
    rows, obs_dev = departures.shape
    owned = rows // lax.axis_size("obs")
    vmem = pl.BlockSpec(memory_space=pltpu.VMEM)
    sums = pl.pallas_call(
        kernel,
        out_shape=pltpu.VMEM((3, 8, 128), jnp.float32),
        in_specs=[pl.BlockSpec(memory_space=pltpu.HBM)] * 6,
        out_specs=vmem,
        scratch_shapes=[
            pltpu.VMEM((rows + 2 * HALO, obs_dev), jnp.bfloat16),
            pltpu.VMEM((2, HALO, obs_dev), jnp.bfloat16),
            pltpu.VMEM(predictors.shape, jnp.bfloat16),
            pltpu.VMEM(inv_band.shape, jnp.bfloat16),
            pltpu.VMEM((band_id.shape[0] // 128, 128), jnp.int32),
            pltpu.SMEM(line_counts.shape, jnp.int32),
            pltpu.VMEM((16, 256), jnp.bfloat16),
            pltpu.VMEM((obs_dev, 256), jnp.bfloat16),
            pltpu.VMEM((16, obs_dev), jnp.bfloat16),
            pltpu.VMEM((32, 128), jnp.float32),
            pltpu.VMEM((16, 256), jnp.float32),
            pltpu.VMEM((2, 128, 256), jnp.bfloat16),
            pltpu.VMEM((2, 128, 256), jnp.bfloat16),
            pltpu.VMEM((BLOCK, 256), jnp.bfloat16),
            pltpu.VMEM((BLOCK, 256), jnp.bfloat16),
            pltpu.VMEM((8, TILES, 8, 128), jnp.bfloat16),
            pltpu.VMEM((8, TILES, 8, 128), jnp.bfloat16),
            pltpu.VMEM((TILES, 8, 128), jnp.float32),
            pltpu.VMEM((8, 3, 8, 128), jnp.float32),
            pltpu.VMEM((8 + len(FAR), 3, 8, 128), jnp.float32),
            pltpu.VMEM((len(FAR), 8, 3, 8, 128), jnp.bfloat16),
            pltpu.VMEM((len(FAR), 8, 3, 8, 128), jnp.bfloat16),
            pltpu.VMEM((len(FAR), 3, 8, 128), jnp.float32),
            pltpu.VMEM((len(FAR), 3, 8, 128), jnp.float32),
            pltpu.SemaphoreType.DMA((5,)),
            pltpu.SemaphoreType.DMA((8,)),
            pltpu.SemaphoreType.DMA((2,)),
            pltpu.SemaphoreType.DMA((2,)),
            pltpu.SemaphoreType.DMA((2,)),
            pltpu.SemaphoreType.DMA,
            pltpu.SemaphoreType.DMA,
            pltpu.SemaphoreType.DMA,
            pltpu.SemaphoreType.DMA,
            pltpu.SemaphoreType.DMA((len(FAR),)),
            pltpu.SemaphoreType.DMA((len(FAR),)),
        ],
        compiler_params=pltpu.CompilerParams(collective_id=0, has_side_effects=True),
        name="normal_equations",
    )(
        departures,
        predictors,
        inv_band,
        band_id.reshape(band_id.shape[0] // 128, 128),
        line_counts,
        jnp.asarray(selectors(), jnp.bfloat16),
    )
    gram, rhs = pl.pallas_call(
        unpack,
        out_shape=(
            jax.ShapeDtypeStruct((owned, PRED * PRED), jnp.float32),
            jax.ShapeDtypeStruct((PRED, owned), jnp.float32),
        ),
        in_specs=[vmem],
        out_specs=(vmem, vmem),
        name="unpack",
    )(pltpu.with_memory_space_constraint(sums, pltpu.VMEM))
    return gram.T, rhs


def solution(mesh):
    in_specs = (P("chan", "obs"), P(None, "obs"), P(None, "chan"), P(), P("obs"))
    out_specs = (P(None, ("chan", "obs")), P(None, ("chan", "obs")))
    return jax.shard_map(
        on_device, mesh=mesh, in_specs=in_specs, out_specs=out_specs, check_vma=False
    )
```

```python
import functools

import jax
import jax.numpy as jnp
import numpy as np
from jax import lax
from jax.experimental import pallas as pl
from jax.experimental.pallas import tpu as pltpu
from jax.sharding import PartitionSpec as P

MESH = pl.DeviceIdType.MESH
PRED = 10
HALO = 32
BLOCK = 256
WINDOW = 192
PAIRS = [(j, k) for j in range(PRED) for k in range(j, PRED)]
HALF = 64
TILES = 19

ORDERS = (
    (2, 5, 4, 3, 1, 6, 7, 0),
    (5, 2, 3, 6, 4, 0, 7, 1),
    (4, 5, 1, 6, 0, 3, 7, 2),
    (1, 5, 6, 0, 2, 4, 7, 3),
    (6, 1, 2, 0, 5, 3, 7, 4),
    (1, 4, 2, 3, 0, 7, 6, 5),
    (3, 1, 2, 5, 0, 4, 7, 6),
    (2, 5, 1, 3, 4, 0, 6, 7),
)
FAR = (4,)


def loads_of(order):
    needed = []
    for block in order:
        for near in (block - 1, block, block + 1):
            if 0 <= near < len(order) and near not in needed:
                needed.append(near)
    return tuple(needed)


def code_of(order):
    return sum(block * 8**n for n, block in enumerate(order))


def pick(z, codes):
    code = jnp.int32(codes[0])
    for n in range(1, len(codes)):
        code = jnp.where(z == n, jnp.int32(codes[n]), code)
    return code


def selectors():
    left = np.zeros((16, 128), np.float32)
    right = np.zeros((16, 128), np.float32)
    for half in range(2):
        for m, (j, k) in enumerate(PAIRS):
            left[j, half * HALF + m] = 1
            right[k, half * HALF + m] = 1
    return np.concatenate([left, right], axis=1)


def kernel(
    dep_ref, pred_hbm, inv_hbm, ids_hbm, lines_hbm, sel_hbm,
    sum_ref,
    cells, edges, pred_ref, inv_ref, ids_ref, lines_ref, sel_ref,
    wq, live_pred, id_rows, id_cols, mat_a, mat_b, weight0, scaled0,
    send1, recv1, own, send2, recv2, far_send, far_recv, far_own, far_sum,
    straight_send, straight_recv, ending,
    small_sem, load_sem, edge_sem, halo_send, halo_recv, send1_sem, recv1_sem, send2_sem, recv2_sem,
    far_send_sem, far_recv_sem, straight_send_sem, straight_recv_sem,
):
    smalls = [
        pltpu.make_async_copy(source, target, small_sem.at[n])
        for n, (source, target) in enumerate(
            [
                (pred_hbm, pred_ref),
                (lines_hbm, lines_ref),
                (sel_hbm, sel_ref),
                (ids_hbm, ids_ref),
                (inv_hbm, inv_ref),
            ]
        )
    ]
    for copy in smalls:
        copy.start()

    obs = lax.axis_index("obs")
    chan = lax.axis_index("chan")
    z, p = obs // 8, obs % 8
    rows = dep_ref.shape[0]
    blocks = rows // BLOCK
    parts = cells.shape[1] // 256
    factor = 1.0 / float(dep_ref.shape[1] * lax.axis_size("obs"))
    last = lax.axis_size("chan") - 1
    order_code = pick(z, [code_of(order + order[:1]) for order in ORDERS])
    load_code = pick(z, [code_of(loads_of(order)) for order in ORDERS])

    barrier = pltpu.get_barrier_semaphore()

    @pl.when(chan > 0)
    def _():
        pl.semaphore_signal(barrier, inc=1, device_id=(obs, chan - 1), device_id_type=MESH)

    @pl.when(chan < last)
    def _():
        pl.semaphore_signal(barrier, inc=1, device_id=(obs, chan + 1), device_id_type=MESH)

    def load(order):
        number = load_code // 8**order % 8
        at = pl.multiple_of(number * BLOCK, BLOCK)
        return pltpu.make_async_copy(
            dep_ref.at[pl.ds(at, BLOCK)],
            cells.at[pl.ds(pl.multiple_of(at + HALO, HALO), BLOCK)],
            load_sem.at[order],
        )

    def edge(n):
        return pltpu.make_async_copy(
            dep_ref.at[pl.ds(n * (rows - HALO), HALO)], edges.at[n], edge_sem.at[n]
        )

    for order in range(blocks):
        load(order).start()
        if order == 2:
            for n in range(2):
                edge(n).start()

    for d in range(1, 8):
        pl.semaphore_signal(barrier, inc=1, device_id=((z + d) % 8 * 8 + p, chan), device_id_type=MESH)
        pl.semaphore_signal(barrier, inc=1, device_id=(z * 8 + (p + d) % 8, chan), device_id_type=MESH)

    @pl.when(z == 0)
    def _():
        for d in range(1, 8):
            for upper in range(1, 8):
                pl.semaphore_signal(
                    barrier, inc=1, device_id=(upper * 8 + (p + d) % 8, chan), device_id_type=MESH
                )

    @pl.when(chan == 0)
    def _():
        cells[pl.ds(0, HALO), :] = jnp.zeros((HALO, cells.shape[1]), jnp.bfloat16)

    @pl.when(chan == last)
    def _():
        cells[pl.ds(HALO + rows, HALO), :] = jnp.zeros((HALO, cells.shape[1]), jnp.bfloat16)

    for copy in smalls:
        copy.wait()

    here = pl.multiple_of(chan * 16, 16)
    id_rows[pl.ds(8, 16), :] = ids_ref[pl.ds(here, 16), :].astype(jnp.float32)
    before = ids_ref[pl.ds(jnp.maximum(here - 1, 0), 1), :].astype(jnp.float32)
    after = ids_ref[pl.ds(jnp.minimum(here + 16, 16 * last + 15), 1), :].astype(jnp.float32)
    id_rows[pl.ds(7, 1), :] = jnp.where(chan > 0, before, -1.0)
    id_rows[pl.ds(24, 1), :] = jnp.where(chan < last, after, -1.0)
    lane16 = lax.broadcasted_iota(jnp.int32, (16, 128), 1)
    turned = [pltpu.roll(id_rows[pl.ds(7 + n, 16), :], 32, axis=1) for n in range(3)]
    id_cols[:, 0:128] = jnp.where(lane16 < 32, turned[0], turned[1])
    id_cols[:, 128:256] = jnp.where(lane16 < 32, turned[1], turned[2])

    def band(first):
        block = first // 128
        entries = inv_ref[:, pl.ds(first, 128)].astype(jnp.float32)
        number = jnp.broadcast_to(id_rows[pl.ds(8 + block, 1), :], (64, 128))
        both = jnp.concatenate([entries, jnp.zeros((1, 128), jnp.float32), number], axis=0).T
        lane = lax.broadcasted_iota(jnp.int32, (128, 128), 1)
        entries = jnp.where(lane < 64, both, 0.0)
        number = jnp.where(lane < 64, pltpu.roll(both, 64, axis=1), both)
        wide = jnp.concatenate([entries, jnp.zeros_like(entries)], axis=1)
        wide = pltpu.roll(wide, 1, axis=1, stride=1, stride_axis=0)
        near = id_cols[pl.ds(block, 1), :]
        same = jnp.concatenate([number, number], axis=1) == near
        return jnp.where(same, wide, 0.0).astype(jnp.bfloat16)

    def start_of(number):
        return pl.multiple_of(number * BLOCK, BLOCK)

    def make(number, mat):
        for n in range(2):
            mat[n] = band(pl.multiple_of(start_of(number) + 128 * n, 128))

    make(order_code % 8, mat_a)

    for s in range(cells.shape[1] // 128):
        lane = lax.broadcasted_iota(jnp.int32, (PRED, 128), 1)
        values = pred_ref[:, s * 128 : s * 128 + 128].astype(jnp.float32)
        values = jnp.where(lane < lines_ref[s], values, 0.0)
        values = jnp.concatenate([values, jnp.zeros((16 - PRED, 128), jnp.float32)], axis=0)
        live_pred[:, s * 128 : s * 128 + 128] = values.astype(jnp.bfloat16)
        picked = jnp.dot(
            values.T.astype(jnp.bfloat16), sel_ref[...], preferred_element_type=jnp.float32
        )
        products = (picked[:, 0:128] * picked[:, 128:256]).astype(jnp.bfloat16)
        wq[pl.ds(s * 128, 128), :] = jnp.concatenate([products, jnp.zeros_like(products)], axis=1)

    def product(number, mat, part):
        first = start_of(number)
        cols = pl.ds(part * 256, 256)
        return [
            jnp.dot(
                mat[n][:, 0:WINDOW],
                cells[pl.ds(pl.multiple_of(first + 128 * n, 128), WINDOW), cols],
                preferred_element_type=jnp.float32,
            )
            for n in range(2)
        ]

    def weigh(weighted):
        weight = [(1.0 / jnp.maximum(jnp.abs(w), 1.0)).astype(jnp.bfloat16) for w in weighted]
        scaled = [jnp.clip(w, -1.0, 1.0).astype(jnp.bfloat16) for w in weighted]
        return jnp.concatenate(weight, axis=0), jnp.concatenate(scaled, axis=0)

    for order in range(3):
        load(order).wait()
    weight0[...], scaled0[...] = weigh(product(order_code % 8, mat_a, 0))

    pl.semaphore_wait(
        barrier, 14 + jnp.minimum(chan, 1) + jnp.minimum(last - chan, 1) + 7 * jnp.minimum(z, 1)
    )

    def up():
        return pltpu.make_async_remote_copy(
            src_ref=edges.at[0],
            dst_ref=cells.at[pl.ds(HALO + rows, HALO)],
            send_sem=halo_send.at[0],
            recv_sem=halo_recv.at[0],
            device_id=(obs, jnp.maximum(chan - 1, 0)),
            device_id_type=MESH,
        )

    def down():
        return pltpu.make_async_remote_copy(
            src_ref=edges.at[1],
            dst_ref=cells.at[pl.ds(0, HALO)],
            send_sem=halo_send.at[1],
            recv_sem=halo_recv.at[1],
            device_id=(obs, jnp.minimum(chan + 1, last)),
            device_id_type=MESH,
        )

    for n in range(2):
        edge(n).wait()

    @pl.when(chan > 0)
    def _():
        up().start()

    @pl.when(chan < last)
    def _():
        down().start()

    def to_plane(number):
        return pltpu.make_async_remote_copy(
            src_ref=send1.at[number],
            dst_ref=recv1.at[z],
            send_sem=send1_sem,
            recv_sem=recv1_sem,
            device_id=(number * 8 + p, chan),
            device_id_type=MESH,
        )

    def split(tiles, target):
        for peer in range(8):
            target[peer, 0:2] = tiles[2 * peer : 2 * peer + 2]
            at = peer % 4 * 32
            low, high = tiles[16 + peer // 4][:, at : at + 32], tiles[18][:, at : at + 32]
            target[peer, 2] = jnp.concatenate([low, high, jnp.zeros((8, 64), jnp.float32)], axis=1)

    def block_step(step, number, following, mat, mat_next):

        for start in range(2):

            @pl.when(step == start)
            def _(start=start):
                for order in range(3 + 3 * start, min(6 + 3 * start, blocks)):
                    load(order).wait()

        @pl.when((following == 0) & (chan > 0))
        def _():
            down().wait_recv()

        @pl.when((following == blocks - 1) & (chan < last))
        def _():
            up().wait_recv()

        make(following, mat_next)
        total = jnp.zeros((BLOCK, 256), jnp.float32)
        sides = jnp.zeros((16, BLOCK), jnp.float32)
        weight, scaled = weight0[...], scaled0[...]
        for part in range(parts):
            if part < parts - 1:
                coming = product(number, mat, part + 1)
            else:
                coming = product(following, mat_next, 0)
            cols = pl.ds(part * 256, 256)
            total = total + jnp.dot(weight, wq[cols, :], preferred_element_type=jnp.float32)
            sides = sides + lax.dot_general(
                live_pred[:, cols], scaled, (((1,), (1,)), ((), ())), preferred_element_type=jnp.float32
            )
            weight, scaled = weigh(coming)
        weight0[...], scaled0[...] = weight, scaled

        lane = lax.broadcasted_iota(jnp.int32, (8, 16, 128), 2)
        halves = total[:, 0:128].reshape(8, 2, 16, 128)
        main = jnp.where(lane < HALF, halves[:, 0], halves[:, 1]).reshape(16, 8, 128)
        own[0:16] = main
        send1[number, 0:16] = main.astype(jnp.bfloat16)
        rest = jnp.concatenate([sides[8:10, 0:128], sides[8:10, 128:256], jnp.zeros((4, 128), jnp.float32)], axis=0)
        for n, tile in enumerate((sides[0:8, 0:128], sides[0:8, 128:256], rest)):
            own[16 + n] = tile
            send1[number, 16 + n] = tile.astype(jnp.bfloat16)

        ahead = (number - z + blocks) % blocks
        straight = (number == 0) & (z > 0)
        near = (ahead > 0) & jnp.logical_not(straight)

        @pl.when(straight)
        def _():
            split(own[...], send2)
            straight_send[...] = send2[...].astype(jnp.bfloat16)

            @pl.loop(0, 8)
            def _(owner):
                pltpu.make_async_remote_copy(
                    src_ref=straight_send.at[owner],
                    dst_ref=straight_recv.at[(z - 1) * 8 + p],
                    send_sem=straight_send_sem,
                    recv_sem=straight_recv_sem,
                    device_id=(owner, chan),
                    device_id_type=MESH,
                ).start()

        for n, distance in enumerate(FAR):
            near = near & (ahead != distance)

            @pl.when((ahead == distance) & jnp.logical_not(straight))
            def _(n=n):
                split(own[...], send2)
                far_send[n] = send2[...].astype(jnp.bfloat16)
                far_own[n] = send2[p]

                @pl.loop(1, 8)
                def _(d):
                    peer = (p + d) % 8
                    pltpu.make_async_remote_copy(
                        src_ref=far_send.at[n, peer],
                        dst_ref=far_recv.at[n, p],
                        send_sem=far_send_sem.at[n],
                        recv_sem=far_recv_sem.at[n],
                        device_id=(z * 8 + peer, chan),
                        device_id_type=MESH,
                    ).start()

        @pl.when(near)
        def _():
            to_plane(number).start()

    def pair(n, code):
        first, second, third = code % 8, code // 8 % 8, code // 64 % 8
        block_step(2 * n, first, second, mat_a, mat_b)
        block_step(2 * n + 1, second, third, mat_b, mat_a)
        return code // 64

    lax.fori_loop(0, blocks // 2, pair, order_code)

    def wait_for(buffer, count, sem):
        pltpu.make_async_copy(buffer.at[pl.ds(0, count)], buffer.at[pl.ds(0, count)], sem).wait()

    def far_copy(n):
        return pltpu.make_async_remote_copy(
            src_ref=far_sum.at[n],
            dst_ref=recv2.at[8 + n],
            send_sem=send2_sem,
            recv_sem=recv2_sem,
            device_id=((z + FAR[n]) % 8 * 8 + p, chan),
            device_id_type=MESH,
        )

    @pl.when(z != 4)
    def _():
        for n in range(len(FAR)):
            wait_for(far_recv.at[n], 7, far_recv_sem.at[n])
            chunk = far_own[n]
            for source in range(8):
                came = far_recv[n, source].astype(jnp.float32)
                chunk = chunk + jnp.where(source == p, jnp.zeros_like(came), came)
            far_sum[n] = chunk
            far_copy(n).start()

    @pl.when(z > 0)
    def _():
        wait_for(recv1, 6, recv1_sem)

    sums = own[...]
    for source in range(8):
        came = recv1[source].astype(jnp.float32)
        away = (z - source + 8) % 8
        absent = (away == 0) | (z == 0)
        for distance in FAR:
            absent = absent | (away == distance)
        sums = sums + jnp.where(absent, jnp.zeros_like(came), came)
    split(sums, send2)

    @pl.loop(1, 8)
    def _(d):
        peer = (p + d) % 8
        pltpu.make_async_remote_copy(
            src_ref=send2.at[peer],
            dst_ref=recv2.at[p],
            send_sem=send2_sem,
            recv_sem=recv2_sem,
            device_id=(z * 8 + peer, chan),
            device_id_type=MESH,
        ).start()

    mine = send2[p]
    @pl.when(z == 0)
    def _():
        wait_for(recv2, 7, recv2_sem)

    @pl.when(z > 0)
    def _():
        wait_for(recv2, 8, recv2_sem)

    whole = mine
    for source in range(8):
        came = recv2[source]
        whole = whole + jnp.where(source == p, jnp.zeros_like(came), came)
    ending[...] = whole

    @pl.when(z > 0)
    def _():
        ending[...] = ending[...] + recv2[8]

    @pl.when(z == 0)
    def _():
        wait_for(straight_recv, 56, straight_recv_sem)
        more = ending[...]
        for source in range(56):
            more = more + straight_recv[source].astype(jnp.float32)
        ending[...] = more

    whole = ending[...]
    rest = whole[2]
    lane = lax.broadcasted_iota(jnp.int32, (8, 128), 1)
    row = lax.broadcasted_iota(jnp.int32, (8, 128), 0)
    moved = pltpu.roll(rest, 6, axis=0)
    sum_ref[0:2] = whole[0:2] * factor
    sum_ref[2] = jnp.where((lane >= 32) & (row < 2) & (p >= 4), moved, rest) * factor

    @pl.when(z % 4 > 0)
    def _():
        wait_for(send1, 5, send1_sem)

    @pl.when(z % 4 == 0)
    def _():
        wait_for(send1, 6, send1_sem)

    @pl.when(z == 4)
    def _():
        wait_for(recv2, 7, send2_sem)

    @pl.when(z != 4)
    def _():
        wait_for(recv2, 8, send2_sem)
        wait_for(far_send.at[0], 7, far_send_sem.at[0])

    @pl.when(z > 0)
    def _():
        wait_for(straight_send, 8, straight_send_sem)

    @pl.when(chan > 0)
    def _():
        up().wait_send()

    @pl.when(chan < last)
    def _():
        down().wait_send()


def unpack(sum_ref, gram_ref, rhs_ref):
    pairs = sum_ref[0:2].reshape(16, 128)
    pairs = jnp.concatenate([pairs, pltpu.roll(pairs, HALF, axis=1)], axis=0)
    entry = lax.broadcasted_iota(jnp.int32, (32, 128), 1)
    left = jnp.zeros_like(entry)
    for n in range(1, PRED):
        left = left + jnp.where(entry >= n * PRED, 1, 0)
    right = entry - left * PRED
    low, high = jnp.minimum(left, right), jnp.maximum(left, right)
    column = jnp.where(entry < PRED * PRED, low * PRED - (low * (low + 1)) // 2 + high, 0)
    spread = jnp.take_along_axis(pairs, column, axis=1, mode="promise_in_bounds")
    gram_ref[...] = spread[:, 0 : PRED * PRED]
    rhs_ref[0:8, :] = sum_ref[2][:, 0:32]
    rhs_ref[8:PRED, :] = sum_ref[2][0 : PRED - 8, 32:64]


def on_device(departures, predictors, inv_band, band_id, line_counts):
    rows, obs_dev = departures.shape
    owned = rows // lax.axis_size("obs")
    vmem = pl.BlockSpec(memory_space=pltpu.VMEM)
    sums = pl.pallas_call(
        kernel,
        out_shape=pltpu.VMEM((3, 8, 128), jnp.float32),
        in_specs=[pl.BlockSpec(memory_space=pltpu.HBM)] * 6,
        out_specs=vmem,
        scratch_shapes=[
            pltpu.VMEM((rows + 2 * HALO, obs_dev), jnp.bfloat16),
            pltpu.VMEM((2, HALO, obs_dev), jnp.bfloat16),
            pltpu.VMEM(predictors.shape, jnp.bfloat16),
            pltpu.VMEM(inv_band.shape, jnp.bfloat16),
            pltpu.VMEM((band_id.shape[0] // 128, 128), jnp.int32),
            pltpu.SMEM(line_counts.shape, jnp.int32),
            pltpu.VMEM((16, 256), jnp.bfloat16),
            pltpu.VMEM((obs_dev, 256), jnp.bfloat16),
            pltpu.VMEM((16, obs_dev), jnp.bfloat16),
            pltpu.VMEM((32, 128), jnp.float32),
            pltpu.VMEM((16, 256), jnp.float32),
            pltpu.VMEM((2, 128, 256), jnp.bfloat16),
            pltpu.VMEM((2, 128, 256), jnp.bfloat16),
            pltpu.VMEM((BLOCK, 256), jnp.bfloat16),
            pltpu.VMEM((BLOCK, 256), jnp.bfloat16),
            pltpu.VMEM((8, TILES, 8, 128), jnp.bfloat16),
            pltpu.VMEM((8, TILES, 8, 128), jnp.bfloat16),
            pltpu.VMEM((TILES, 8, 128), jnp.float32),
            pltpu.VMEM((8, 3, 8, 128), jnp.float32),
            pltpu.VMEM((8 + len(FAR), 3, 8, 128), jnp.float32),
            pltpu.VMEM((len(FAR), 8, 3, 8, 128), jnp.bfloat16),
            pltpu.VMEM((len(FAR), 8, 3, 8, 128), jnp.bfloat16),
            pltpu.VMEM((len(FAR), 3, 8, 128), jnp.float32),
            pltpu.VMEM((len(FAR), 3, 8, 128), jnp.float32),
            pltpu.VMEM((8, 3, 8, 128), jnp.bfloat16),
            pltpu.VMEM((56, 3, 8, 128), jnp.bfloat16),
            pltpu.VMEM((3, 8, 128), jnp.float32),
            pltpu.SemaphoreType.DMA((5,)),
            pltpu.SemaphoreType.DMA((8,)),
            pltpu.SemaphoreType.DMA((2,)),
            pltpu.SemaphoreType.DMA((2,)),
            pltpu.SemaphoreType.DMA((2,)),
            pltpu.SemaphoreType.DMA,
            pltpu.SemaphoreType.DMA,
            pltpu.SemaphoreType.DMA,
            pltpu.SemaphoreType.DMA,
            pltpu.SemaphoreType.DMA((len(FAR),)),
            pltpu.SemaphoreType.DMA((len(FAR),)),
            pltpu.SemaphoreType.DMA,
            pltpu.SemaphoreType.DMA,
        ],
        compiler_params=pltpu.CompilerParams(collective_id=0, has_side_effects=True),
        name="normal_equations",
    )(
        departures,
        predictors,
        inv_band,
        band_id.reshape(band_id.shape[0] // 128, 128),
        line_counts,
        jnp.asarray(selectors(), jnp.bfloat16),
    )
    gram, rhs = pl.pallas_call(
        unpack,
        out_shape=(
            jax.ShapeDtypeStruct((owned, PRED * PRED), jnp.float32),
            jax.ShapeDtypeStruct((PRED, owned), jnp.float32),
        ),
        in_specs=[vmem],
        out_specs=(vmem, vmem),
        name="unpack",
    )(pltpu.with_memory_space_constraint(sums, pltpu.VMEM))
    return gram.T, rhs


def solution(mesh):
    in_specs = (P("chan", "obs"), P(None, "obs"), P(None, "chan"), P(), P("obs"))
    out_specs = (P(None, ("chan", "obs")), P(None, ("chan", "obs")))
    return jax.shard_map(
        on_device, mesh=mesh, in_specs=in_specs, out_specs=out_specs, check_vma=False
    )
```

```python
import functools

import jax
import jax.numpy as jnp
import numpy as np
from jax import lax
from jax.experimental import pallas as pl
from jax.experimental.pallas import tpu as pltpu
from jax.sharding import PartitionSpec as P

MESH = pl.DeviceIdType.MESH
PRED = 10
HALO = 32
BLOCK = 256
WINDOW = 192
PAIRS = [(j, k) for j in range(PRED) for k in range(j, PRED)]
HALF = 64
TILES = 19

ORDERS = (
    (2, 5, 4, 3, 1, 6, 7, 0),
    (5, 2, 3, 0, 6, 4, 7, 1),
    (4, 5, 1, 0, 6, 3, 7, 2),
    (1, 5, 6, 0, 2, 4, 7, 3),
    (6, 1, 2, 0, 5, 3, 7, 4),
    (1, 4, 2, 0, 3, 7, 6, 5),
    (3, 1, 2, 0, 5, 4, 7, 6),
    (2, 5, 1, 0, 3, 4, 6, 7),
)
FAR = (4,)


def loads_of(order):
    needed = []
    for block in order:
        for near in (block - 1, block, block + 1):
            if 0 <= near < len(order) and near not in needed:
                needed.append(near)
    return tuple(needed)


def code_of(order):
    return sum(block * 8**n for n, block in enumerate(order))


def pick(z, codes):
    code = jnp.int32(codes[0])
    for n in range(1, len(codes)):
        code = jnp.where(z == n, jnp.int32(codes[n]), code)
    return code


def selectors():
    left = np.zeros((16, 128), np.float32)
    right = np.zeros((16, 128), np.float32)
    for half in range(2):
        for m, (j, k) in enumerate(PAIRS):
            left[j, half * HALF + m] = 1
            right[k, half * HALF + m] = 1
    return np.concatenate([left, right], axis=1)


def kernel(
    dep_ref, pred_hbm, inv_hbm, ids_hbm, lines_hbm, sel_hbm,
    sum_ref,
    cells, edges, pred_ref, inv_ref, ids_ref, lines_ref, sel_ref,
    wq, live_pred, id_rows, id_cols, mat_a, mat_b, weight0, scaled0,
    send1, recv1, own, send2, recv2, far_send, far_recv, far_own, far_sum,
    straight_send, straight_recv, ending,
    small_sem, load_sem, edge_sem, halo_send, halo_recv, send1_sem, recv1_sem, send2_sem, recv2_sem,
    far_send_sem, far_recv_sem, straight_send_sem, straight_recv_sem,
):
    smalls = [
        pltpu.make_async_copy(source, target, small_sem.at[n])
        for n, (source, target) in enumerate(
            [
                (pred_hbm, pred_ref),
                (lines_hbm, lines_ref),
                (sel_hbm, sel_ref),
                (ids_hbm, ids_ref),
                (inv_hbm, inv_ref),
            ]
        )
    ]
    for copy in smalls:
        copy.start()

    obs = lax.axis_index("obs")
    chan = lax.axis_index("chan")
    z, p = obs // 8, obs % 8
    rows = dep_ref.shape[0]
    blocks = rows // BLOCK
    parts = cells.shape[1] // 256
    factor = 1.0 / float(dep_ref.shape[1] * lax.axis_size("obs"))
    last = lax.axis_size("chan") - 1
    order_code = pick(z, [code_of(order + order[:1]) for order in ORDERS])
    load_code = pick(z, [code_of(loads_of(order)) for order in ORDERS])

    barrier = pltpu.get_barrier_semaphore()

    @pl.when(chan > 0)
    def _():
        pl.semaphore_signal(barrier, inc=1, device_id=(obs, chan - 1), device_id_type=MESH)

    @pl.when(chan < last)
    def _():
        pl.semaphore_signal(barrier, inc=1, device_id=(obs, chan + 1), device_id_type=MESH)

    def load(order):
        number = load_code // 8**order % 8
        at = pl.multiple_of(number * BLOCK, BLOCK)
        return pltpu.make_async_copy(
            dep_ref.at[pl.ds(at, BLOCK)],
            cells.at[pl.ds(pl.multiple_of(at + HALO, HALO), BLOCK)],
            load_sem.at[order],
        )

    def edge(n):
        return pltpu.make_async_copy(
            dep_ref.at[pl.ds(n * (rows - HALO), HALO)], edges.at[n], edge_sem.at[n]
        )

    for order in range(blocks):
        load(order).start()
        if order == 2:
            for n in range(2):
                edge(n).start()

    for d in range(1, 8):
        pl.semaphore_signal(barrier, inc=1, device_id=((z + d) % 8 * 8 + p, chan), device_id_type=MESH)
        pl.semaphore_signal(barrier, inc=1, device_id=(z * 8 + (p + d) % 8, chan), device_id_type=MESH)

    @pl.when(z == 0)
    def _():
        for d in range(1, 8):
            for upper in range(1, 8):
                pl.semaphore_signal(
                    barrier, inc=1, device_id=(upper * 8 + (p + d) % 8, chan), device_id_type=MESH
                )

    @pl.when(chan == 0)
    def _():
        cells[pl.ds(0, HALO), :] = jnp.zeros((HALO, cells.shape[1]), jnp.bfloat16)

    @pl.when(chan == last)
    def _():
        cells[pl.ds(HALO + rows, HALO), :] = jnp.zeros((HALO, cells.shape[1]), jnp.bfloat16)

    for copy in smalls:
        copy.wait()

    here = pl.multiple_of(chan * 16, 16)
    id_rows[pl.ds(8, 16), :] = ids_ref[pl.ds(here, 16), :].astype(jnp.float32)
    before = ids_ref[pl.ds(jnp.maximum(here - 1, 0), 1), :].astype(jnp.float32)
    after = ids_ref[pl.ds(jnp.minimum(here + 16, 16 * last + 15), 1), :].astype(jnp.float32)
    id_rows[pl.ds(7, 1), :] = jnp.where(chan > 0, before, -1.0)
    id_rows[pl.ds(24, 1), :] = jnp.where(chan < last, after, -1.0)
    lane16 = lax.broadcasted_iota(jnp.int32, (16, 128), 1)
    turned = [pltpu.roll(id_rows[pl.ds(7 + n, 16), :], 32, axis=1) for n in range(3)]
    id_cols[:, 0:128] = jnp.where(lane16 < 32, turned[0], turned[1])
    id_cols[:, 128:256] = jnp.where(lane16 < 32, turned[1], turned[2])

    def band(first):
        block = first // 128
        entries = inv_ref[:, pl.ds(first, 128)].astype(jnp.float32)
        number = jnp.broadcast_to(id_rows[pl.ds(8 + block, 1), :], (64, 128))
        both = jnp.concatenate([entries, jnp.zeros((1, 128), jnp.float32), number], axis=0).T
        lane = lax.broadcasted_iota(jnp.int32, (128, 128), 1)
        entries = jnp.where(lane < 64, both, 0.0)
        number = jnp.where(lane < 64, pltpu.roll(both, 64, axis=1), both)
        wide = jnp.concatenate([entries, jnp.zeros_like(entries)], axis=1)
        wide = pltpu.roll(wide, 1, axis=1, stride=1, stride_axis=0)
        near = id_cols[pl.ds(block, 1), :]
        same = jnp.concatenate([number, number], axis=1) == near
        return jnp.where(same, wide, 0.0).astype(jnp.bfloat16)

    def start_of(number):
        return pl.multiple_of(number * BLOCK, BLOCK)

    def make(number, mat):
        for n in range(2):
            mat[n] = band(pl.multiple_of(start_of(number) + 128 * n, 128))

    make(order_code % 8, mat_a)

    for s in range(cells.shape[1] // 128):
        lane = lax.broadcasted_iota(jnp.int32, (PRED, 128), 1)
        values = pred_ref[:, s * 128 : s * 128 + 128].astype(jnp.float32)
        values = jnp.where(lane < lines_ref[s], values, 0.0)
        values = jnp.concatenate([values, jnp.zeros((16 - PRED, 128), jnp.float32)], axis=0)
        live_pred[:, s * 128 : s * 128 + 128] = values.astype(jnp.bfloat16)
        picked = jnp.dot(
            values.T.astype(jnp.bfloat16), sel_ref[...], preferred_element_type=jnp.float32
        )
        products = (picked[:, 0:128] * picked[:, 128:256]).astype(jnp.bfloat16)
        wq[pl.ds(s * 128, 128), :] = jnp.concatenate([products, jnp.zeros_like(products)], axis=1)

    def one(number, mat, part, n):
        return jnp.dot(
            mat[n][:, 0:WINDOW],
            cells[
                pl.ds(pl.multiple_of(start_of(number) + 128 * n, 128), WINDOW), pl.ds(part * 256, 256)
            ],
            preferred_element_type=jnp.float32,
        )

    def product(number, mat, part):
        first = start_of(number)
        cols = pl.ds(part * 256, 256)
        return [
            jnp.dot(
                mat[n][:, 0:WINDOW],
                cells[pl.ds(pl.multiple_of(first + 128 * n, 128), WINDOW), cols],
                preferred_element_type=jnp.float32,
            )
            for n in range(2)
        ]

    def weigh(weighted):
        weight = [(1.0 / jnp.maximum(jnp.abs(w), 1.0)).astype(jnp.bfloat16) for w in weighted]
        scaled = [jnp.clip(w, -1.0, 1.0).astype(jnp.bfloat16) for w in weighted]
        return jnp.concatenate(weight, axis=0), jnp.concatenate(scaled, axis=0)

    for order in range(3):
        load(order).wait()
    weight0[...], scaled0[...] = weigh(product(order_code % 8, mat_a, 0))

    pl.semaphore_wait(
        barrier, 14 + jnp.minimum(chan, 1) + jnp.minimum(last - chan, 1) + 7 * jnp.minimum(z, 1)
    )

    def up():
        return pltpu.make_async_remote_copy(
            src_ref=edges.at[0],
            dst_ref=cells.at[pl.ds(HALO + rows, HALO)],
            send_sem=halo_send.at[0],
            recv_sem=halo_recv.at[0],
            device_id=(obs, jnp.maximum(chan - 1, 0)),
            device_id_type=MESH,
        )

    def down():
        return pltpu.make_async_remote_copy(
            src_ref=edges.at[1],
            dst_ref=cells.at[pl.ds(0, HALO)],
            send_sem=halo_send.at[1],
            recv_sem=halo_recv.at[1],
            device_id=(obs, jnp.minimum(chan + 1, last)),
            device_id_type=MESH,
        )

    for n in range(2):
        edge(n).wait()

    @pl.when(chan > 0)
    def _():
        up().start()

    @pl.when(chan < last)
    def _():
        down().start()

    def to_plane(number):
        return pltpu.make_async_remote_copy(
            src_ref=send1.at[number],
            dst_ref=recv1.at[z],
            send_sem=send1_sem,
            recv_sem=recv1_sem,
            device_id=(number * 8 + p, chan),
            device_id_type=MESH,
        )

    def split(tiles, target):
        for peer in range(8):
            target[peer, 0:2] = tiles[2 * peer : 2 * peer + 2]
            at = peer % 4 * 32
            low, high = tiles[16 + peer // 4][:, at : at + 32], tiles[18][:, at : at + 32]
            target[peer, 2] = jnp.concatenate([low, high, jnp.zeros((8, 64), jnp.float32)], axis=1)

    def block_step(step, number, following, mat, mat_next):

        for start in range(2):

            @pl.when(step == start)
            def _(start=start):
                for order in range(3 + 3 * start, min(6 + 3 * start, blocks)):
                    load(order).wait()

        @pl.when((following == 0) & (chan > 0))
        def _():
            down().wait_recv()

        @pl.when((following == blocks - 1) & (chan < last))
        def _():
            up().wait_recv()

        make(following, mat_next)
        total = jnp.zeros((BLOCK, 256), jnp.float32)
        sides = jnp.zeros((16, BLOCK), jnp.float32)
        weight, scaled = weight0[...], scaled0[...]
        for part in range(parts):
            cols = pl.ds(part * 256, 256)
            at, block, using = (part + 1, number, mat) if part < parts - 1 else (0, following, mat_next)
            coming = []
            coming.append(one(block, using, at, 0))
            coming.append(one(block, using, at, 1))
            sides = sides + lax.dot_general(
                live_pred[:, cols], scaled, (((1,), (1,)), ((), ())), preferred_element_type=jnp.float32
            )
            total = total + jnp.dot(weight, wq[cols, :], preferred_element_type=jnp.float32)
            weight, scaled = weigh(coming)
        weight0[...], scaled0[...] = weight, scaled

        lane = lax.broadcasted_iota(jnp.int32, (8, 16, 128), 2)
        halves = total[:, 0:128].reshape(8, 2, 16, 128)
        main = jnp.where(lane < HALF, halves[:, 0], halves[:, 1]).reshape(16, 8, 128)
        own[0:16] = main
        send1[number, 0:16] = main.astype(jnp.bfloat16)
        rest = jnp.concatenate([sides[8:10, 0:128], sides[8:10, 128:256], jnp.zeros((4, 128), jnp.float32)], axis=0)
        for n, tile in enumerate((sides[0:8, 0:128], sides[0:8, 128:256], rest)):
            own[16 + n] = tile
            send1[number, 16 + n] = tile.astype(jnp.bfloat16)

        ahead = (number - z + blocks) % blocks
        straight = (number == 0) & (z > 0)
        near = (ahead > 0) & jnp.logical_not(straight)

        @pl.when(straight)
        def _():
            split(own[...], send2)
            straight_send[...] = send2[...].astype(jnp.bfloat16)

            @pl.loop(0, 8)
            def _(owner):
                pltpu.make_async_remote_copy(
                    src_ref=straight_send.at[owner],
                    dst_ref=straight_recv.at[(z - 1) * 8 + p],
                    send_sem=straight_send_sem,
                    recv_sem=straight_recv_sem,
                    device_id=(owner, chan),
                    device_id_type=MESH,
                ).start()

        for n, distance in enumerate(FAR):
            near = near & (ahead != distance)

            @pl.when((ahead == distance) & jnp.logical_not(straight))
            def _(n=n):
                split(own[...], send2)
                far_send[n] = send2[...].astype(jnp.bfloat16)
                far_own[n] = send2[p]

                @pl.loop(1, 8)
                def _(d):
                    peer = (p + d) % 8
                    pltpu.make_async_remote_copy(
                        src_ref=far_send.at[n, peer],
                        dst_ref=far_recv.at[n, p],
                        send_sem=far_send_sem.at[n],
                        recv_sem=far_recv_sem.at[n],
                        device_id=(z * 8 + peer, chan),
                        device_id_type=MESH,
                    ).start()

        @pl.when(near)
        def _():
            to_plane(number).start()

    def pair(n, code):
        first, second, third = code % 8, code // 8 % 8, code // 64 % 8
        block_step(2 * n, first, second, mat_a, mat_b)
        block_step(2 * n + 1, second, third, mat_b, mat_a)
        return code // 64

    lax.fori_loop(0, blocks // 2, pair, order_code)

    def wait_for(buffer, count, sem):
        pltpu.make_async_copy(buffer.at[pl.ds(0, count)], buffer.at[pl.ds(0, count)], sem).wait()

    def far_copy(n):
        return pltpu.make_async_remote_copy(
            src_ref=far_sum.at[n],
            dst_ref=recv2.at[8 + n],
            send_sem=send2_sem,
            recv_sem=recv2_sem,
            device_id=((z + FAR[n]) % 8 * 8 + p, chan),
            device_id_type=MESH,
        )

    @pl.when(z != 4)
    def _():
        for n in range(len(FAR)):
            wait_for(far_recv.at[n], 7, far_recv_sem.at[n])
            chunk = far_own[n]
            for source in range(8):
                came = far_recv[n, source].astype(jnp.float32)
                chunk = chunk + jnp.where(source == p, jnp.zeros_like(came), came)
            far_sum[n] = chunk
            far_copy(n).start()

    @pl.when(z > 0)
    def _():
        wait_for(recv1, 6, recv1_sem)

    sums = own[...]
    for source in range(8):
        came = recv1[source].astype(jnp.float32)
        away = (z - source + 8) % 8
        absent = (away == 0) | (z == 0)
        for distance in FAR:
            absent = absent | (away == distance)
        sums = sums + jnp.where(absent, jnp.zeros_like(came), came)
    split(sums, send2)

    @pl.loop(1, 8)
    def _(d):
        peer = (p + d) % 8
        pltpu.make_async_remote_copy(
            src_ref=send2.at[peer],
            dst_ref=recv2.at[p],
            send_sem=send2_sem,
            recv_sem=recv2_sem,
            device_id=(z * 8 + peer, chan),
            device_id_type=MESH,
        ).start()

    mine = send2[p]
    @pl.when(z == 0)
    def _():
        wait_for(recv2, 7, recv2_sem)

    @pl.when(z > 0)
    def _():
        wait_for(recv2, 8, recv2_sem)

    whole = mine
    for source in range(8):
        came = recv2[source]
        whole = whole + jnp.where(source == p, jnp.zeros_like(came), came)
    ending[...] = whole

    @pl.when(z > 0)
    def _():
        ending[...] = ending[...] + recv2[8]

    @pl.when(z == 0)
    def _():
        wait_for(straight_recv, 56, straight_recv_sem)
        more = ending[...]
        for source in range(56):
            more = more + straight_recv[source].astype(jnp.float32)
        ending[...] = more

    whole = ending[...]
    rest = whole[2]
    lane = lax.broadcasted_iota(jnp.int32, (8, 128), 1)
    row = lax.broadcasted_iota(jnp.int32, (8, 128), 0)
    moved = pltpu.roll(rest, 6, axis=0)
    sum_ref[0:2] = whole[0:2] * factor
    sum_ref[2] = jnp.where((lane >= 32) & (row < 2) & (p >= 4), moved, rest) * factor

    @pl.when(z % 4 > 0)
    def _():
        wait_for(send1, 5, send1_sem)

    @pl.when(z % 4 == 0)
    def _():
        wait_for(send1, 6, send1_sem)

    @pl.when(z == 4)
    def _():
        wait_for(recv2, 7, send2_sem)

    @pl.when(z != 4)
    def _():
        wait_for(recv2, 8, send2_sem)
        wait_for(far_send.at[0], 7, far_send_sem.at[0])

    @pl.when(z > 0)
    def _():
        wait_for(straight_send, 8, straight_send_sem)

    @pl.when(chan > 0)
    def _():
        up().wait_send()

    @pl.when(chan < last)
    def _():
        down().wait_send()


def unpack(sum_ref, gram_ref, rhs_ref):
    pairs = sum_ref[0:2].reshape(16, 128)
    pairs = jnp.concatenate([pairs, pltpu.roll(pairs, HALF, axis=1)], axis=0)
    entry = lax.broadcasted_iota(jnp.int32, (32, 128), 1)
    left = jnp.zeros_like(entry)
    for n in range(1, PRED):
        left = left + jnp.where(entry >= n * PRED, 1, 0)
    right = entry - left * PRED
    low, high = jnp.minimum(left, right), jnp.maximum(left, right)
    column = jnp.where(entry < PRED * PRED, low * PRED - (low * (low + 1)) // 2 + high, 0)
    spread = jnp.take_along_axis(pairs, column, axis=1, mode="promise_in_bounds")
    gram_ref[...] = spread[:, 0 : PRED * PRED]
    rhs_ref[0:8, :] = sum_ref[2][:, 0:32]
    rhs_ref[8:PRED, :] = sum_ref[2][0 : PRED - 8, 32:64]


def on_device(departures, predictors, inv_band, band_id, line_counts):
    rows, obs_dev = departures.shape
    owned = rows // lax.axis_size("obs")
    vmem = pl.BlockSpec(memory_space=pltpu.VMEM)
    sums = pl.pallas_call(
        kernel,
        out_shape=pltpu.VMEM((3, 8, 128), jnp.float32),
        in_specs=[pl.BlockSpec(memory_space=pltpu.HBM)] * 6,
        out_specs=vmem,
        scratch_shapes=[
            pltpu.VMEM((rows + 2 * HALO, obs_dev), jnp.bfloat16),
            pltpu.VMEM((2, HALO, obs_dev), jnp.bfloat16),
            pltpu.VMEM(predictors.shape, jnp.bfloat16),
            pltpu.VMEM(inv_band.shape, jnp.bfloat16),
            pltpu.VMEM((band_id.shape[0] // 128, 128), jnp.int32),
            pltpu.SMEM(line_counts.shape, jnp.int32),
            pltpu.VMEM((16, 256), jnp.bfloat16),
            pltpu.VMEM((obs_dev, 256), jnp.bfloat16),
            pltpu.VMEM((16, obs_dev), jnp.bfloat16),
            pltpu.VMEM((32, 128), jnp.float32),
            pltpu.VMEM((16, 256), jnp.float32),
            pltpu.VMEM((2, 128, 256), jnp.bfloat16),
            pltpu.VMEM((2, 128, 256), jnp.bfloat16),
            pltpu.VMEM((BLOCK, 256), jnp.bfloat16),
            pltpu.VMEM((BLOCK, 256), jnp.bfloat16),
            pltpu.VMEM((8, TILES, 8, 128), jnp.bfloat16),
            pltpu.VMEM((8, TILES, 8, 128), jnp.bfloat16),
            pltpu.VMEM((TILES, 8, 128), jnp.float32),
            pltpu.VMEM((8, 3, 8, 128), jnp.float32),
            pltpu.VMEM((8 + len(FAR), 3, 8, 128), jnp.float32),
            pltpu.VMEM((len(FAR), 8, 3, 8, 128), jnp.bfloat16),
            pltpu.VMEM((len(FAR), 8, 3, 8, 128), jnp.bfloat16),
            pltpu.VMEM((len(FAR), 3, 8, 128), jnp.float32),
            pltpu.VMEM((len(FAR), 3, 8, 128), jnp.float32),
            pltpu.VMEM((8, 3, 8, 128), jnp.bfloat16),
            pltpu.VMEM((56, 3, 8, 128), jnp.bfloat16),
            pltpu.VMEM((3, 8, 128), jnp.float32),
            pltpu.SemaphoreType.DMA((5,)),
            pltpu.SemaphoreType.DMA((8,)),
            pltpu.SemaphoreType.DMA((2,)),
            pltpu.SemaphoreType.DMA((2,)),
            pltpu.SemaphoreType.DMA((2,)),
            pltpu.SemaphoreType.DMA,
            pltpu.SemaphoreType.DMA,
            pltpu.SemaphoreType.DMA,
            pltpu.SemaphoreType.DMA,
            pltpu.SemaphoreType.DMA((len(FAR),)),
            pltpu.SemaphoreType.DMA((len(FAR),)),
            pltpu.SemaphoreType.DMA,
            pltpu.SemaphoreType.DMA,
        ],
        compiler_params=pltpu.CompilerParams(collective_id=0, has_side_effects=True),
        name="normal_equations",
    )(
        departures,
        predictors,
        inv_band,
        band_id.reshape(band_id.shape[0] // 128, 128),
        line_counts,
        jnp.asarray(selectors(), jnp.bfloat16),
    )
    gram, rhs = pl.pallas_call(
        unpack,
        out_shape=(
            jax.ShapeDtypeStruct((owned, PRED * PRED), jnp.float32),
            jax.ShapeDtypeStruct((PRED, owned), jnp.float32),
        ),
        in_specs=[vmem],
        out_specs=(vmem, vmem),
        name="unpack",
    )(pltpu.with_memory_space_constraint(sums, pltpu.VMEM))
    return gram.T, rhs


def solution(mesh):
    in_specs = (P("chan", "obs"), P(None, "obs"), P(None, "chan"), P(), P("obs"))
    out_specs = (P(None, ("chan", "obs")), P(None, ("chan", "obs")))
    return jax.shard_map(
        on_device, mesh=mesh, in_specs=in_specs, out_specs=out_specs, check_vma=False
    )
```

```python
import functools

import jax
import jax.numpy as jnp
import numpy as np
from jax import lax
from jax.experimental import pallas as pl
from jax.experimental.pallas import tpu as pltpu
from jax.sharding import PartitionSpec as P

MESH = pl.DeviceIdType.MESH
PRED = 10
HALO = 32
BLOCK = 256
WINDOW = 192
PAIRS = [(j, k) for j in range(PRED) for k in range(j, PRED)]
HALF = 64
TILES = 19

ORDERS = (
    (2, 5, 4, 3, 1, 6, 7, 0),
    (5, 2, 3, 0, 6, 4, 7, 1),
    (4, 5, 1, 0, 6, 3, 7, 2),
    (1, 5, 6, 0, 2, 4, 7, 3),
    (6, 1, 2, 0, 5, 3, 7, 4),
    (1, 4, 2, 0, 3, 7, 6, 5),
    (3, 1, 2, 0, 5, 4, 7, 6),
    (2, 5, 1, 0, 3, 4, 6, 7),
)
FAR = (4,)


def loads_of(order):
    needed = []
    for block in order:
        for near in (block - 1, block, block + 1):
            if 0 <= near < len(order) and near not in needed:
                needed.append(near)
    return tuple(needed)


def code_of(order):
    return sum(block * 8**n for n, block in enumerate(order))


def pick(z, codes):
    code = jnp.int32(codes[0])
    for n in range(1, len(codes)):
        code = jnp.where(z == n, jnp.int32(codes[n]), code)
    return code


def selectors():
    left = np.zeros((16, 128), np.float32)
    right = np.zeros((16, 128), np.float32)
    for half in range(2):
        for m, (j, k) in enumerate(PAIRS):
            left[j, half * HALF + m] = 1
            right[k, half * HALF + m] = 1
    return np.concatenate([left, right], axis=1)


def kernel(
    dep_ref, pred_hbm, inv_hbm, ids_hbm, lines_hbm, sel_hbm,
    sum_ref,
    cells, edges, pred_ref, inv_ref, ids_ref, lines_ref, sel_ref,
    wq, live_pred, id_rows, id_cols, mat_a, mat_b, weight0, scaled0,
    send1, recv1, own, send2, recv2, far_send, far_recv, far_own, far_sum,
    straight_send, straight_recv, ending,
    small_sem, load_sem, edge_sem, halo_send, halo_recv, send1_sem, recv1_sem, send2_sem, recv2_sem,
    far_send_sem, far_recv_sem, straight_send_sem, straight_recv_sem,
):
    smalls = [
        pltpu.make_async_copy(source, target, small_sem.at[n])
        for n, (source, target) in enumerate(
            [
                (pred_hbm, pred_ref),
                (lines_hbm, lines_ref),
                (sel_hbm, sel_ref),
                (ids_hbm, ids_ref),
                (inv_hbm, inv_ref),
            ]
        )
    ]
    for copy in smalls:
        copy.start()

    obs = lax.axis_index("obs")
    chan = lax.axis_index("chan")
    z, p = obs // 8, obs % 8
    rows = dep_ref.shape[0]
    blocks = rows // BLOCK
    parts = cells.shape[1] // 256
    factor = 1.0 / float(dep_ref.shape[1] * lax.axis_size("obs"))
    last = lax.axis_size("chan") - 1
    order_code = pick(z, [code_of(order + order[:1]) for order in ORDERS])
    load_code = pick(z, [code_of(loads_of(order)) for order in ORDERS])

    barrier = pltpu.get_barrier_semaphore()

    @pl.when(chan > 0)
    def _():
        pl.semaphore_signal(barrier, inc=1, device_id=(obs, chan - 1), device_id_type=MESH)

    @pl.when(chan < last)
    def _():
        pl.semaphore_signal(barrier, inc=1, device_id=(obs, chan + 1), device_id_type=MESH)

    def load(order):
        number = load_code // 8**order % 8
        at = pl.multiple_of(number * BLOCK, BLOCK)
        return pltpu.make_async_copy(
            dep_ref.at[pl.ds(at, BLOCK)],
            cells.at[pl.ds(pl.multiple_of(at + HALO, HALO), BLOCK)],
            load_sem.at[order],
        )

    def edge(n):
        return pltpu.make_async_copy(
            dep_ref.at[pl.ds(n * (rows - HALO), HALO)], edges.at[n], edge_sem.at[n]
        )

    for order in range(blocks):
        load(order).start()
        if order == 2:
            for n in range(2):
                edge(n).start()

    for d in range(1, 8):
        pl.semaphore_signal(barrier, inc=1, device_id=((z + d) % 8 * 8 + p, chan), device_id_type=MESH)
        pl.semaphore_signal(barrier, inc=1, device_id=(z * 8 + (p + d) % 8, chan), device_id_type=MESH)

    @pl.when(z == 0)
    def _():
        for d in range(1, 8):
            for upper in range(1, 8):
                pl.semaphore_signal(
                    barrier, inc=1, device_id=(upper * 8 + (p + d) % 8, chan), device_id_type=MESH
                )

    @pl.when(chan == 0)
    def _():
        cells[pl.ds(0, HALO), :] = jnp.zeros((HALO, cells.shape[1]), jnp.bfloat16)

    @pl.when(chan == last)
    def _():
        cells[pl.ds(HALO + rows, HALO), :] = jnp.zeros((HALO, cells.shape[1]), jnp.bfloat16)

    for copy in smalls:
        copy.wait()

    here = pl.multiple_of(chan * 16, 16)
    id_rows[pl.ds(8, 16), :] = ids_ref[pl.ds(here, 16), :].astype(jnp.float32)
    before = ids_ref[pl.ds(jnp.maximum(here - 1, 0), 1), :].astype(jnp.float32)
    after = ids_ref[pl.ds(jnp.minimum(here + 16, 16 * last + 15), 1), :].astype(jnp.float32)
    id_rows[pl.ds(7, 1), :] = jnp.where(chan > 0, before, -1.0)
    id_rows[pl.ds(24, 1), :] = jnp.where(chan < last, after, -1.0)
    lane16 = lax.broadcasted_iota(jnp.int32, (16, 128), 1)
    turned = [pltpu.roll(id_rows[pl.ds(7 + n, 16), :], 32, axis=1) for n in range(3)]
    id_cols[:, 0:128] = jnp.where(lane16 < 32, turned[0], turned[1])
    id_cols[:, 128:256] = jnp.where(lane16 < 32, turned[1], turned[2])

    def band(first):
        block = first // 128
        entries = inv_ref[:, pl.ds(first, 128)].astype(jnp.float32)
        number = jnp.broadcast_to(id_rows[pl.ds(8 + block, 1), :], (64, 128))
        both = jnp.concatenate([entries, jnp.zeros((1, 128), jnp.float32), number], axis=0).T
        lane = lax.broadcasted_iota(jnp.int32, (128, 128), 1)
        entries = jnp.where(lane < 64, both, 0.0)
        number = jnp.where(lane < 64, pltpu.roll(both, 64, axis=1), both)
        wide = jnp.concatenate([entries, jnp.zeros_like(entries)], axis=1)
        wide = pltpu.roll(wide, 1, axis=1, stride=1, stride_axis=0)
        near = id_cols[pl.ds(block, 1), :]
        same = jnp.concatenate([number, number], axis=1) == near
        return jnp.where(same, wide, 0.0).astype(jnp.bfloat16)

    def start_of(number):
        return pl.multiple_of(number * BLOCK, BLOCK)

    def make(number, mat):
        for n in range(2):
            mat[n] = band(pl.multiple_of(start_of(number) + 128 * n, 128))

    make(order_code % 8, mat_a)

    for s in range(cells.shape[1] // 128):
        lane = lax.broadcasted_iota(jnp.int32, (PRED, 128), 1)
        values = pred_ref[:, s * 128 : s * 128 + 128].astype(jnp.float32)
        values = jnp.where(lane < lines_ref[s], values, 0.0)
        values = jnp.concatenate([values, jnp.zeros((16 - PRED, 128), jnp.float32)], axis=0)
        live_pred[:, s * 128 : s * 128 + 128] = values.astype(jnp.bfloat16)
        picked = jnp.dot(
            values.T.astype(jnp.bfloat16), sel_ref[...], preferred_element_type=jnp.float32
        )
        products = (picked[:, 0:128] * picked[:, 128:256]).astype(jnp.bfloat16)
        wq[pl.ds(s * 128, 128), :] = jnp.concatenate([products, jnp.zeros_like(products)], axis=1)

    def one(number, mat, part, n):
        return jnp.dot(
            mat[n][:, 0:WINDOW],
            cells[
                pl.ds(pl.multiple_of(start_of(number) + 128 * n, 128), WINDOW), pl.ds(part * 256, 256)
            ],
            preferred_element_type=jnp.float32,
        )

    def product(number, mat, part):
        first = start_of(number)
        cols = pl.ds(part * 256, 256)
        return [
            jnp.dot(
                mat[n][:, 0:WINDOW],
                cells[pl.ds(pl.multiple_of(first + 128 * n, 128), WINDOW), cols],
                preferred_element_type=jnp.float32,
            )
            for n in range(2)
        ]

    def weigh(weighted):
        weight = [(1.0 / jnp.maximum(jnp.abs(w), 1.0)).astype(jnp.bfloat16) for w in weighted]
        scaled = [jnp.clip(w, -1.0, 1.0).astype(jnp.bfloat16) for w in weighted]
        return jnp.concatenate(weight, axis=0), jnp.concatenate(scaled, axis=0)

    for order in range(3):
        load(order).wait()
    weight0[...], scaled0[...] = weigh(product(order_code % 8, mat_a, 0))

    pl.semaphore_wait(
        barrier, 14 + jnp.minimum(chan, 1) + jnp.minimum(last - chan, 1) + 7 * jnp.minimum(z, 1)
    )

    def up():
        return pltpu.make_async_remote_copy(
            src_ref=edges.at[0],
            dst_ref=cells.at[pl.ds(HALO + rows, HALO)],
            send_sem=halo_send.at[0],
            recv_sem=halo_recv.at[0],
            device_id=(obs, jnp.maximum(chan - 1, 0)),
            device_id_type=MESH,
        )

    def down():
        return pltpu.make_async_remote_copy(
            src_ref=edges.at[1],
            dst_ref=cells.at[pl.ds(0, HALO)],
            send_sem=halo_send.at[1],
            recv_sem=halo_recv.at[1],
            device_id=(obs, jnp.minimum(chan + 1, last)),
            device_id_type=MESH,
        )

    for n in range(2):
        edge(n).wait()

    @pl.when(chan > 0)
    def _():
        up().start()

    @pl.when(chan < last)
    def _():
        down().start()

    def to_plane(number):
        return pltpu.make_async_remote_copy(
            src_ref=send1.at[number],
            dst_ref=recv1.at[z],
            send_sem=send1_sem,
            recv_sem=recv1_sem,
            device_id=(number * 8 + p, chan),
            device_id_type=MESH,
        )

    def split(tiles, target):
        for peer in range(8):
            target[peer, 0:2] = tiles[2 * peer : 2 * peer + 2]
            at = peer % 4 * 32
            low, high = tiles[16 + peer // 4][:, at : at + 32], tiles[18][:, at : at + 32]
            target[peer, 2] = jnp.concatenate([low, high, jnp.zeros((8, 64), jnp.float32)], axis=1)

    def block_step(step, number, following, mat, mat_next):

        for start in range(2):

            @pl.when(step == start)
            def _(start=start):
                for order in range(3 + 3 * start, min(6 + 3 * start, blocks)):
                    load(order).wait()

        @pl.when((following == 0) & (chan > 0))
        def _():
            down().wait_recv()

        @pl.when((following == blocks - 1) & (chan < last))
        def _():
            up().wait_recv()

        make(following, mat_next)
        total = jnp.zeros((BLOCK, 256), jnp.float32)
        sides = jnp.zeros((16, BLOCK), jnp.float32)
        weight, scaled = weight0[...], scaled0[...]
        for part in range(parts):
            cols = pl.ds(part * 256, 256)
            at, block, using = (part + 1, number, mat) if part < parts - 1 else (0, following, mat_next)
            coming = []
            coming.append(one(block, using, at, 0))
            coming.append(one(block, using, at, 1))
            sides = sides + lax.dot_general(
                live_pred[:, cols], scaled, (((1,), (1,)), ((), ())), preferred_element_type=jnp.float32
            )
            total = total + jnp.dot(weight, wq[cols, :], preferred_element_type=jnp.float32)
            weight, scaled = weigh(coming)
        weight0[...], scaled0[...] = weight, scaled

        lane = lax.broadcasted_iota(jnp.int32, (8, 16, 128), 2)
        halves = total[:, 0:128].reshape(8, 2, 16, 128)
        main = jnp.where(lane < HALF, halves[:, 0], halves[:, 1]).reshape(16, 8, 128)
        own[0:16] = main
        send1[number, 0:16] = main.astype(jnp.bfloat16)
        rest = jnp.concatenate([sides[8:10, 0:128], sides[8:10, 128:256], jnp.zeros((4, 128), jnp.float32)], axis=0)
        for n, tile in enumerate((sides[0:8, 0:128], sides[0:8, 128:256], rest)):
            own[16 + n] = tile
            send1[number, 16 + n] = tile.astype(jnp.bfloat16)

        ahead = (number - z + blocks) % blocks
        straight = (number == 0) & (z > 0)
        near = (ahead > 0) & jnp.logical_not(straight)

        @pl.when(straight)
        def _():
            split(own[...], send2)
            straight_send[...] = send2[...].astype(jnp.bfloat16)

            @pl.loop(0, 8)
            def _(owner):
                pltpu.make_async_remote_copy(
                    src_ref=straight_send.at[owner],
                    dst_ref=straight_recv.at[(z - 1) * 8 + p],
                    send_sem=straight_send_sem,
                    recv_sem=straight_recv_sem,
                    device_id=(owner, chan),
                    device_id_type=MESH,
                ).start()

        for n, distance in enumerate(FAR):
            near = near & (ahead != distance)

            @pl.when((ahead == distance) & jnp.logical_not(straight))
            def _(n=n):
                split(own[...], send2)
                far_send[n] = send2[...].astype(jnp.bfloat16)
                far_own[n] = send2[p]

                @pl.loop(1, 8)
                def _(d):
                    peer = (p + d) % 8
                    pltpu.make_async_remote_copy(
                        src_ref=far_send.at[n, peer],
                        dst_ref=far_recv.at[n, p],
                        send_sem=far_send_sem.at[n],
                        recv_sem=far_recv_sem.at[n],
                        device_id=(z * 8 + peer, chan),
                        device_id_type=MESH,
                    ).start()

        @pl.when(near)
        def _():
            to_plane(number).start()

    def pair(n, code):
        first, second, third = code % 8, code // 8 % 8, code // 64 % 8
        block_step(2 * n, first, second, mat_a, mat_b)
        block_step(2 * n + 1, second, third, mat_b, mat_a)
        return code // 64

    lax.fori_loop(0, blocks // 2, pair, order_code)

    def wait_for(buffer, count, sem):
        pltpu.make_async_copy(buffer.at[pl.ds(0, count)], buffer.at[pl.ds(0, count)], sem).wait()

    def far_copy(n):
        return pltpu.make_async_remote_copy(
            src_ref=far_sum.at[n],
            dst_ref=recv2.at[8 + n],
            send_sem=send2_sem,
            recv_sem=recv2_sem,
            device_id=((z + FAR[n]) % 8 * 8 + p, chan),
            device_id_type=MESH,
        )

    def pass_far_on():
        for n in range(len(FAR)):
            wait_for(far_recv.at[n], 7, far_recv_sem.at[n])
            chunk = far_own[n]
            for source in range(8):
                came = far_recv[n, source].astype(jnp.float32)
                chunk = chunk + jnp.where(source == p, jnp.zeros_like(came), came)
            far_sum[n] = chunk
            far_copy(n).start()

    @pl.when(z > 4)
    def _():
        pass_far_on()

    @pl.when(z > 0)
    def _():
        wait_for(recv1, 6, recv1_sem)

    sums = own[...]
    for source in range(8):
        came = recv1[source].astype(jnp.float32)
        away = (z - source + 8) % 8
        absent = (away == 0) | (z == 0)
        for distance in FAR:
            absent = absent | (away == distance)
        sums = sums + jnp.where(absent, jnp.zeros_like(came), came)
    split(sums, send2)

    @pl.loop(1, 8)
    def _(d):
        peer = (p + d) % 8
        pltpu.make_async_remote_copy(
            src_ref=send2.at[peer],
            dst_ref=recv2.at[p],
            send_sem=send2_sem,
            recv_sem=recv2_sem,
            device_id=(z * 8 + peer, chan),
            device_id_type=MESH,
        ).start()

    @pl.when(z < 4)
    def _():
        pass_far_on()

    mine = send2[p]
    @pl.when(z == 0)
    def _():
        wait_for(recv2, 7, recv2_sem)

    @pl.when(z > 0)
    def _():
        wait_for(recv2, 8, recv2_sem)

    whole = mine
    for source in range(8):
        came = recv2[source]
        whole = whole + jnp.where(source == p, jnp.zeros_like(came), came)
    ending[...] = whole

    @pl.when(z > 0)
    def _():
        ending[...] = ending[...] + recv2[8]

    @pl.when(z == 0)
    def _():
        wait_for(straight_recv, 56, straight_recv_sem)
        more = ending[...]
        for source in range(56):
            more = more + straight_recv[source].astype(jnp.float32)
        ending[...] = more

    whole = ending[...]
    rest = whole[2]
    lane = lax.broadcasted_iota(jnp.int32, (8, 128), 1)
    row = lax.broadcasted_iota(jnp.int32, (8, 128), 0)
    moved = pltpu.roll(rest, 6, axis=0)
    sum_ref[0:2] = whole[0:2] * factor
    sum_ref[2] = jnp.where((lane >= 32) & (row < 2) & (p >= 4), moved, rest) * factor

    @pl.when(z % 4 > 0)
    def _():
        wait_for(send1, 5, send1_sem)

    @pl.when(z % 4 == 0)
    def _():
        wait_for(send1, 6, send1_sem)

    @pl.when(z == 4)
    def _():
        wait_for(recv2, 7, send2_sem)

    @pl.when(z != 4)
    def _():
        wait_for(recv2, 8, send2_sem)
        wait_for(far_send.at[0], 7, far_send_sem.at[0])

    @pl.when(z > 0)
    def _():
        wait_for(straight_send, 8, straight_send_sem)

    @pl.when(chan > 0)
    def _():
        up().wait_send()

    @pl.when(chan < last)
    def _():
        down().wait_send()


def unpack(sum_ref, gram_ref, rhs_ref):
    pairs = sum_ref[0:2].reshape(16, 128)
    pairs = jnp.concatenate([pairs, pltpu.roll(pairs, HALF, axis=1)], axis=0)
    entry = lax.broadcasted_iota(jnp.int32, (32, 128), 1)
    left = jnp.zeros_like(entry)
    for n in range(1, PRED):
        left = left + jnp.where(entry >= n * PRED, 1, 0)
    right = entry - left * PRED
    low, high = jnp.minimum(left, right), jnp.maximum(left, right)
    column = jnp.where(entry < PRED * PRED, low * PRED - (low * (low + 1)) // 2 + high, 0)
    spread = jnp.take_along_axis(pairs, column, axis=1, mode="promise_in_bounds")
    gram_ref[...] = spread[:, 0 : PRED * PRED]
    rhs_ref[0:8, :] = sum_ref[2][:, 0:32]
    rhs_ref[8:PRED, :] = sum_ref[2][0 : PRED - 8, 32:64]


def on_device(departures, predictors, inv_band, band_id, line_counts):
    rows, obs_dev = departures.shape
    owned = rows // lax.axis_size("obs")
    vmem = pl.BlockSpec(memory_space=pltpu.VMEM)
    sums = pl.pallas_call(
        kernel,
        out_shape=pltpu.VMEM((3, 8, 128), jnp.float32),
        in_specs=[pl.BlockSpec(memory_space=pltpu.HBM)] * 6,
        out_specs=vmem,
        scratch_shapes=[
            pltpu.VMEM((rows + 2 * HALO, obs_dev), jnp.bfloat16),
            pltpu.VMEM((2, HALO, obs_dev), jnp.bfloat16),
            pltpu.VMEM(predictors.shape, jnp.bfloat16),
            pltpu.VMEM(inv_band.shape, jnp.bfloat16),
            pltpu.VMEM((band_id.shape[0] // 128, 128), jnp.int32),
            pltpu.SMEM(line_counts.shape, jnp.int32),
            pltpu.VMEM((16, 256), jnp.bfloat16),
            pltpu.VMEM((obs_dev, 256), jnp.bfloat16),
            pltpu.VMEM((16, obs_dev), jnp.bfloat16),
            pltpu.VMEM((32, 128), jnp.float32),
            pltpu.VMEM((16, 256), jnp.float32),
            pltpu.VMEM((2, 128, 256), jnp.bfloat16),
            pltpu.VMEM((2, 128, 256), jnp.bfloat16),
            pltpu.VMEM((BLOCK, 256), jnp.bfloat16),
            pltpu.VMEM((BLOCK, 256), jnp.bfloat16),
            pltpu.VMEM((8, TILES, 8, 128), jnp.bfloat16),
            pltpu.VMEM((8, TILES, 8, 128), jnp.bfloat16),
            pltpu.VMEM((TILES, 8, 128), jnp.float32),
            pltpu.VMEM((8, 3, 8, 128), jnp.float32),
            pltpu.VMEM((8 + len(FAR), 3, 8, 128), jnp.float32),
            pltpu.VMEM((len(FAR), 8, 3, 8, 128), jnp.bfloat16),
            pltpu.VMEM((len(FAR), 8, 3, 8, 128), jnp.bfloat16),
            pltpu.VMEM((len(FAR), 3, 8, 128), jnp.float32),
            pltpu.VMEM((len(FAR), 3, 8, 128), jnp.float32),
            pltpu.VMEM((8, 3, 8, 128), jnp.bfloat16),
            pltpu.VMEM((56, 3, 8, 128), jnp.bfloat16),
            pltpu.VMEM((3, 8, 128), jnp.float32),
            pltpu.SemaphoreType.DMA((5,)),
            pltpu.SemaphoreType.DMA((8,)),
            pltpu.SemaphoreType.DMA((2,)),
            pltpu.SemaphoreType.DMA((2,)),
            pltpu.SemaphoreType.DMA((2,)),
            pltpu.SemaphoreType.DMA,
            pltpu.SemaphoreType.DMA,
            pltpu.SemaphoreType.DMA,
            pltpu.SemaphoreType.DMA,
            pltpu.SemaphoreType.DMA((len(FAR),)),
            pltpu.SemaphoreType.DMA((len(FAR),)),
            pltpu.SemaphoreType.DMA,
            pltpu.SemaphoreType.DMA,
        ],
        compiler_params=pltpu.CompilerParams(collective_id=0, has_side_effects=True),
        name="normal_equations",
    )(
        departures,
        predictors,
        inv_band,
        band_id.reshape(band_id.shape[0] // 128, 128),
        line_counts,
        jnp.asarray(selectors(), jnp.bfloat16),
    )
    gram, rhs = pl.pallas_call(
        unpack,
        out_shape=(
            jax.ShapeDtypeStruct((owned, PRED * PRED), jnp.float32),
            jax.ShapeDtypeStruct((PRED, owned), jnp.float32),
        ),
        in_specs=[vmem],
        out_specs=(vmem, vmem),
        name="unpack",
    )(pltpu.with_memory_space_constraint(sums, pltpu.VMEM))
    return gram.T, rhs


def solution(mesh):
    in_specs = (P("chan", "obs"), P(None, "obs"), P(None, "chan"), P(), P("obs"))
    out_specs = (P(None, ("chan", "obs")), P(None, ("chan", "obs")))
    return jax.shard_map(
        on_device, mesh=mesh, in_specs=in_specs, out_specs=out_specs, check_vma=False
    )
```
